32 devices in a mesh: wave: 8 (over y, x, core), lev: 4 (over z).
Axes of the slice: x: 2, y: 2, z: 4, core: 2. Of those that a mesh axis runs over, the one named last changes fastest.
Arguments:
- spec: bfloat16 [16, 128, 640], P('wave', 'lev'), may hold values from -1.5 to 1.5
- legendre: bfloat16 [16, 1280, 640], P('wave'), may hold values from -0.25 to 0.25
- layer_depth_share: float32 [16], P('lev'), may hold values from 0.5 to 2
- quad_weight: float32 [1280], replicated, may hold values from 8 to 32
- wave_of_slot: int32 [16], P('wave'), may hold values from 0 to 639, as said below
Outputs:
- tendency: bfloat16 [16, 128, 640], P('wave', 'lev')
The draws below stay inside these ranges and needn't reach their ends.
Inputs may be any that keep to these rules, and one draw needn't show every extreme that they name: `wave_of_slot`: slots 2 i and 2 i + 1 hold wavenumbers m and 639 - m; no wavenumber appears twice.
All inputs are finite; a program needn't handle non-finite values.
Results may differ from the reference program's by a relative error of at most 0.0047.
The reference program's roundings to bfloat16 on the way count: a program that leaves them out, or rounds other values in their place, can miss the bound.
Values may be sent and summed in bfloat16 or wider, within the bound.
A program may use at most 128 MiB of HBM per device.

```python
import math
import jax
import jax.numpy as jnp
from jax import lax

LAT = 1280
ORDER_SPAN = 640
QUANTITY_TOTAL = 4
EASTWARD_MODES = 16
LEVELS = 16
COLS = 128
MAXLON = 2576
N_LEV = 4


def draw_wave_of_slot(key, part):
    chosen = jax.random.permutation(key, ORDER_SPAN // 2)[:EASTWARD_MODES // 2].astype(jnp.int32)
    return jnp.stack([chosen, ORDER_SPAN - 1 - chosen], axis=1).reshape(EASTWARD_MODES)


def level_of(own_key, shape, cuts, smallest, high):
    gain, own = 1.0, jax.random.fold_in(own_key, 6)
    for dim, parts in cuts:
        draws = jnp.exp(jax.random.uniform(jax.random.fold_in(own, dim), (parts,), jnp.float32, smallest / len(cuts), high / len(cuts)))
        gain = gain * jnp.repeat(draws, shape[dim] // parts).reshape([-1 if axis == dim else 1 for axis in range(len(shape))])
    return gain


def noise(key, shape, scale, reach, pieces=(), kind=jnp.bfloat16):
    level = level_of(key, shape, pieces, -0.22, 0.18) if pieces else 1.0
    values = jax.random.normal(key, shape, jnp.float32) * scale * level
    return jnp.minimum(jnp.maximum(values, -reach), reach).astype(kind)


def setup_inputs(seed: int = 0) -> dict:
    key_of = jax.random.split(jax.random.key(seed), 6)
    spec = noise(key_of[0], (EASTWARD_MODES, COLS, ORDER_SPAN), EASTWARD_MODES ** -0.5, 1.5, ((0, 8), (1, 4)))
    legendre = noise(key_of[1], (EASTWARD_MODES, LAT, ORDER_SPAN), ORDER_SPAN ** -0.5, 0.25, ((0, 8),))
    layer_depth_share = jnp.clip(jnp.exp(math.log(2.0) - 1.3862944 * jax.random.uniform(key_of[2], (LEVELS,), jnp.float32) ** level_of(key_of[2], (LEVELS,), ((0, 4),), -0.2, 0.2)), 0.5, 2.0)
    quad_weight = jnp.clip(jnp.exp(jax.random.uniform(key_of[3], (LAT,), jnp.float32, math.log(8.0), math.log(32.0))), 8.0, 32.0)
    wave_of_slot = draw_wave_of_slot(jax.random.fold_in(key_of[5], 71), 0)
    return {"spec": spec, "legendre": legendre, "layer_depth_share": layer_depth_share, "quad_weight": quad_weight, "wave_of_slot": wave_of_slot}


full_turn = 2.0 * math.pi


def rate_bundle(eastward_velocity, northward_velocity, local_curl_spin, thermal_state, planetary_rotation_effect, processor_dimension):
    absolute = local_curl_spin + planetary_rotation_effect
    return jnp.stack([absolute * eastward_velocity, absolute * northward_velocity,
                      0.5 * (eastward_velocity * eastward_velocity + northward_velocity * northward_velocity),
                      eastward_velocity * thermal_state], axis=processor_dimension)


def reference(spec, legendre, layer_depth_share, quad_weight, wave_of_slot):
    layers_on_processor = LEVELS // N_LEV
    degree_index = jnp.arange(ORDER_SPAN, dtype=jnp.int32)
    valid_cols = degree_index[None, :] < (ORDER_SPAN - wave_of_slot)[:, None]
    screened_entries = jnp.where(valid_cols[:, None, :], spec, jnp.zeros_like(spec))

    def inverse_one(inputs):
        leg_table, coeffs = inputs
        return jnp.dot(leg_table, coeffs.T, preferred_element_type=jnp.float32).astype(jnp.bfloat16)

    fourier = jnp.moveaxis(lax.map(inverse_one, (legendre, screened_entries)), 1, 0)
    points = jnp.arange(MAXLON, dtype=jnp.int32)
    weight_two = jnp.where(wave_of_slot == 0, 1.0, 2.0).astype(jnp.float32)

    def grid_one(inputs):
        latitude, coeffs = inputs
        length = 20 + 4 * jnp.minimum(latitude, LAT - 1 - latitude)
        length_f = length.astype(jnp.float32)
        phase_int = (wave_of_slot[:, None] * points[None, :]) % length
        angles = phase_int.astype(jnp.float32) * full_turn / length_f
        cosine = jnp.cos(angles)
        sine_vals = jnp.sin(angles)
        resolved = 2 * wave_of_slot < length
        amplitude = jnp.where(resolved, weight_two, 0.0)[:, None]
        split_parts = coeffs.reshape(EASTWARD_MODES, N_LEV, 2, QUANTITY_TOTAL, layers_on_processor)
        real_part = split_parts[:, :, 0].reshape(EASTWARD_MODES, -1)
        imag_part = split_parts[:, :, 1].reshape(EASTWARD_MODES, -1)
        grid_vals = jnp.dot(real_part.T, (amplitude * cosine).astype(jnp.bfloat16), preferred_element_type=jnp.float32)
        grid_vals = grid_vals - jnp.dot(imag_part.T, (amplitude * sine_vals).astype(jnp.bfloat16), preferred_element_type=jnp.float32)
        grid_vals = grid_vals.reshape(N_LEV, QUANTITY_TOTAL, layers_on_processor, MAXLON)
        planetary_rotation_effect = 2.0 * jnp.cos((latitude.astype(jnp.float32) + 0.5) * (math.pi / LAT))
        products = rate_bundle(grid_vals[:, 0], grid_vals[:, 1], grid_vals[:, 2], grid_vals[:, 3], planetary_rotation_effect, 1)
        products = products.astype(jnp.bfloat16).reshape(N_LEV * QUANTITY_TOTAL * layers_on_processor, MAXLON)
        live_mask = (points[None, :] < length) & resolved[:, None]
        cos_back = jnp.where(live_mask, cosine, 0.0).astype(jnp.bfloat16)
        sin_back = jnp.where(live_mask, sine_vals, 0.0).astype(jnp.bfloat16)
        row_scale = quad_weight[latitude] / length_f
        real_back = jnp.dot(products, cos_back.T, preferred_element_type=jnp.float32) * row_scale
        imag_back = -jnp.dot(products, sin_back.T, preferred_element_type=jnp.float32) * row_scale
        merged = jnp.stack([real_back.T.reshape(EASTWARD_MODES, N_LEV, QUANTITY_TOTAL, layers_on_processor),
                            imag_back.T.reshape(EASTWARD_MODES, N_LEV, QUANTITY_TOTAL, layers_on_processor)], axis=2)
        return merged.reshape(EASTWARD_MODES, COLS).astype(jnp.bfloat16)

    tend_rows = lax.map(grid_one, (jnp.arange(LAT, dtype=jnp.int32), fourier))

    def direct_one(inputs):
        leg_table, coeffs = inputs
        return jnp.dot(coeffs.T, leg_table, preferred_element_type=jnp.float32)

    tendency = lax.map(direct_one, (legendre, jnp.moveaxis(tend_rows, 1, 0)))
    thermal_state = screened_entries.reshape(EASTWARD_MODES, N_LEV, 2, QUANTITY_TOTAL, layers_on_processor, ORDER_SPAN)[:, :, :, 3].astype(jnp.float32)
    scaled_entries = thermal_state * layer_depth_share.reshape(N_LEV, 1, layers_on_processor, 1)
    scaled_entries = jnp.moveaxis(scaled_entries, 2, 1).reshape(EASTWARD_MODES, 2, LEVELS, ORDER_SPAN)
    below_sum = jnp.flip(jnp.cumsum(jnp.flip(scaled_entries, 2), 2), 2)
    geopot = jnp.moveaxis(below_sum.reshape(EASTWARD_MODES, 2, N_LEV, layers_on_processor, ORDER_SPAN), 1, 2)
    tendency = tendency.reshape(EASTWARD_MODES, N_LEV, 2, QUANTITY_TOTAL, layers_on_processor, ORDER_SPAN)
    tendency = tendency.at[:, :, :, 2].add(geopot)
    tendency = jnp.where(valid_cols[:, None, None, None, None, :], tendency, 0.0)
    return tendency.reshape(EASTWARD_MODES, COLS, ORDER_SPAN).astype(jnp.bfloat16)
```

```python
import functools
import math

import jax
import jax.numpy as jnp
import numpy as np
from jax import lax
from jax.experimental import pallas as pl
from jax.experimental.pallas import tpu as pltpu
from jax.sharding import PartitionSpec as P

LANES = 128
POINTS = 2 * LANES
UNROLL = 4
NT = (((1,), (1,)), ((), ()))


def taylor(first, count):
    return [(-1.0) ** k / math.factorial(2 * k + first) for k in range(count)]


def horner(square, terms):
    total = jnp.full_like(square, terms[-1])
    for term in reversed(terms[:-1]):
        total = total * square + term
    return total


def turn_trig(steps, length, inverse):
    whole = jnp.floor(steps * inverse + 0.5)
    angle = (steps - whole * length) * inverse * (2.0 * math.pi)
    square = angle * angle
    return horner(square, taylor(0, 10)), angle * horner(square, taylor(1, 10))


def lane_maps(slots, fields, layers):
    order = np.arange(slots * 2 * 2 * fields * layers)
    natural = order.reshape(slots, 2, 2, fields, layers)
    return natural.transpose(0, 2, 3, 1, 4).reshape(-1)


def fourier_stage(dims, spec_ref, leg_ref, loads, live, gain, perm_ref, rows_ref):
    slots, columns, half = dims["slots"], dims["columns"], dims["half"]
    total = jnp.zeros((half, LANES), jnp.float32)
    for slot in range(slots):
        masked = spec_ref[slot] * live[slot].astype(jnp.bfloat16)
        for hemi in range(2):
            at = (slot * 2 + hemi) * columns
            pieces = []
            if at:
                pieces.append(jnp.zeros((at, masked.shape[1]), masked.dtype))
            pieces.append(masked)
            if at + columns < LANES:
                pieces.append(jnp.zeros((LANES - at - columns, masked.shape[1]), masked.dtype))
            loads[slot * 2 + hemi].wait()
            total += lax.dot_general(
                leg_ref[slot, hemi * half : (hemi + 1) * half, :],
                jnp.concatenate(pieces, 0),
                NT,
                preferred_element_type=jnp.float32,
            )
    rows = jnp.dot(total.astype(jnp.bfloat16), perm_ref[...], preferred_element_type=jnp.float32)
    rows_ref[...] = rows * gain


def split_rows(dims, rows_ref, send_ref):
    quarter, half = dims["quarter"], dims["half"]
    for place in range(dims["groups"]):
        low = rows_ref[place * quarter : (place + 1) * quarter, :]
        top = half - place * quarter
        high = rows_ref[top - quarter : top, :]
        send_ref[place] = jnp.concatenate([low, high], 0).astype(jnp.bfloat16)


def whereabouts(dims, device, number):
    quarter, block = dims["quarter"], dims["block"]
    local = [number * block + u for u in range(block)]
    dist = [
        jnp.where(
            r < quarter, device * quarter + r, dims["half"] - (device + 2) * quarter + r
        )
        for r in local
    ]
    lengths = [20 + 4 * q for q in dist]
    return local, dist, lengths, [length.astype(jnp.float32) for length in lengths]


def tiles_of(longest):
    return (longest // 2 + POINTS) // POINTS


def most_tiles(dims):
    quarter, block, half = dims["quarter"], dims["block"], dims["half"]
    most = 0
    for device in range(dims["groups"]):
        total = 0
        for number in range(2 * quarter // block):
            r = number * block + block - 1
            q = device * quarter + r if r < quarter else half - (device + 2) * quarter + r
            total += tiles_of(20 + 4 * q)
        most = max(most, total)
    return most


def back_home(dims, part, slot, u):
    width = 2 * dims["waves"]
    if width >= LANES:
        return u * width + part * dims["waves"] + slot * dims["groups"]
    share = LANES // width
    inner = (part * dims["slots"] + slot) * share + u % share
    return u // share * LANES + inner * dims["groups"]


def table_stage(dims, device, waves, quad_ref, cor_ref, scratch):
    slots, groups, half = dims["slots"], dims["groups"], dims["half"]
    fields, layers, block = dims["fields"], dims["layers"], dims["block"]
    state, hop, tab, back_tab, cor, scale = scratch
    total_lat = 2 * half
    pair = min(2, block)
    wide = slots * block * groups
    lane = lax.broadcasted_iota(jnp.int32, (groups, LANES), 1).astype(jnp.float32)
    north_row = lax.broadcasted_iota(jnp.int32, (2 * layers, LANES), 0) < layers
    wave_row = lax.broadcasted_iota(jnp.int32, (2 * layers, POINTS), 0) < layers
    width = 2 * dims["waves"]
    column = lax.broadcasted_iota(jnp.int32, (2 * layers, POINTS), 1)
    if width >= LANES:
        owner = column // width
    else:
        share = LANES // width
        owner = column // LANES * share + column // groups % share

    def group(number, first):
        local, dist, lengths, floats = whereabouts(dims, device, number)
        scaled = jnp.zeros((2 * layers, POINTS), jnp.float32)
        for u, length in enumerate(floats):
            inverse = 1.0 / jnp.full((groups, LANES), length, jnp.float32)
            for slot in range(slots):
                begin = turn_trig(waves[slot] * lane, length, inverse)
                cosine = jnp.broadcast_to(begin[0][:, LANES // 2 : LANES // 2 + 1], (groups, LANES))
                sine = jnp.broadcast_to(begin[1][:, LANES // 2 : LANES // 2 + 1], (groups, LANES))
                keep = jnp.where(2.0 * waves[slot] < length, 1.0, 0.0)
                at = (slot * block + u) * groups
                state[0, at : at + groups, :] = begin[0] * keep
                state[1, at : at + groups, :] = begin[1] * keep
                hop[0, at : at + groups, :] = cosine * cosine - sine * sine
                hop[1, at : at + groups, :] = 2.0 * cosine * sine
            cor[number, u * 2 * layers : (u + 1) * 2 * layers, :] = jnp.where(
                north_row, cor_ref[dist[u]], cor_ref[total_lat - 1 - dist[u]]
            )
            here = jnp.where(wave_row, quad_ref[dist[u]], quad_ref[total_lat - 1 - dist[u]])
            scaled = jnp.where(owner == u, here / length, scaled)
        scale[number] = scaled

        def tile(index, item):
            for side in range(POINTS // LANES):
                cols = slice(side * LANES, (side + 1) * LANES)
                point = lane + (index * POINTS + side * LANES).astype(jnp.float32)
                start = jnp.minimum(point + 0.5, 1.0)
                weight = [
                    jnp.maximum(jnp.minimum(0.5 * length + 0.5 - point, start), 0.0)
                    for length in floats
                ]
                for u in range(0, block, pair):
                    both = jnp.concatenate(weight[u : u + pair], 0).astype(jnp.bfloat16)
                    for slot in range(slots):
                        at = (slot * block + u) * groups
                        rows = slice(at, at + pair * groups)
                        cosine, sine = state[0, rows, :], state[1, rows, :]
                        turn_cos, turn_sin = hop[0, rows, :], hop[1, rows, :]
                        state[0, rows, :] = cosine * turn_cos - sine * turn_sin
                        state[1, rows, :] = sine * turn_cos + cosine * turn_sin
                        for part, value in enumerate((cosine, sine)):
                            packed = value.astype(jnp.bfloat16)
                            put = part * wide + at
                            tab[item, put : put + pair * groups, cols] = packed
                            put = back_home(dims, part, slot, u)
                            back_tab[item, put : put + pair * groups, cols] = packed * both
            return item + 1

        return lax.fori_loop(0, tiles_of(lengths[-1]), tile, first)

    lax.fori_loop(0, 2 * dims["quarter"] // block, group, 0)


def coefficient_stage(dims, get_ref, base, total):
    slots, groups, layers = dims["slots"], dims["groups"], dims["layers"]
    fields, block, count = dims["fields"], dims["block"], 2 * dims["quarter"]
    width = fields * 2 * layers
    number = count // block
    lane = lax.broadcasted_iota(jnp.int32, (groups, LANES), 1)
    south_lane = lane // layers % 2 == 1
    first_slot = lax.broadcasted_iota(jnp.int32, (width, LANES), 1) < block * groups
    eye = (
        lax.broadcasted_iota(jnp.int32, (LANES, LANES), 0)
        == lax.broadcasted_iota(jnp.int32, (LANES, LANES), 1)
    ).astype(jnp.bfloat16)
    for start in range(0, number, 2):
        pieces = []
        for n in range(start, min(start + 2, number)):
            both = []
            for u in range(block):
                at = n * block + u
                north = get_ref[pl.ds(at, groups, stride=count), :]
                south = get_ref[pl.ds(count - 1 - at, groups, stride=count), :]
                both.append(jnp.where(south_lane, south, north))
            pieces += both * (LANES // (block * groups))
        turned = lax.dot_general(
            eye,
            jnp.concatenate(pieces, 0).astype(jnp.bfloat16),
            NT,
            preferred_element_type=jnp.float32,
        )
        for n in range(start, min(start + 2, number)):
            mine = turned[:, (n - start) * LANES : (n - start + 1) * LANES]
            for part in range(2):
                value = [
                    mine[(slot * 2 + part) * width : (slot * 2 + part + 1) * width]
                    for slot in range(slots)
                ]
                base[n, :, part * LANES : (part + 1) * LANES] = jnp.where(
                    first_slot, value[0], value[1]
                ).astype(jnp.bfloat16)
    total[...] = jnp.zeros_like(total)


def item_stage(dims, device, base, tab, back_tab, cor, total):
    groups, layers, block = dims["groups"], dims["layers"], dims["block"]
    fields, number = dims["fields"], 2 * dims["quarter"] // dims["block"]
    width = fields * 2 * layers
    rows = 2 * width
    ends = []
    for n in range(number):
        lengths = whereabouts(dims, device, n)[2]
        ends.append(tiles_of(lengths[-1]) + (ends[-1] if ends else 0))
    lane = lax.broadcasted_iota(jnp.int32, (width, LANES), 1)
    mine = [
        (lane // groups % block == u).astype(jnp.float32).astype(jnp.bfloat16)
        for u in range(block)
    ]
    span = 2 * dims["waves"]
    share = max(1, LANES // span)
    reach = max(LANES, span)
    across = lax.broadcasted_iota(jnp.int32, (width, reach), 1)
    sign = jnp.where(across // (reach // 2) == 0, 1.0, -1.0)

    def one(item):
        n = 0
        for end in ends:
            n = n + jnp.where(item >= end, 1, 0)
        real = base[n, :, :LANES]
        imag = base[n, :, LANES:]
        pieces = []
        for u in range(block):
            left, right = real * mine[u], imag * mine[u]
            pieces.append(jnp.concatenate([left, -right], 1))
            pieces.append(jnp.concatenate([left, right], 1))
        grid = jnp.dot(
            jnp.concatenate(pieces, 0), tab[item], preferred_element_type=jnp.float32
        )
        made = []
        for u in range(block):
            extra = cor[n, u * 2 * layers : (u + 1) * 2 * layers, :]
            extra = jnp.concatenate([extra] * (POINTS // LANES), 1)
            for side in range(2):
                at = (u * 2 + side) * width
                part = [
                    grid[at + f * 2 * layers : at + (f + 1) * 2 * layers] for f in range(fields)
                ]
                absolute = part[2] + extra
                made += [
                    absolute * part[0],
                    absolute * part[1],
                    0.5 * (part[0] * part[0] + part[1] * part[1]),
                    part[0] * part[3],
                ]
        products = jnp.concatenate(made, 0).astype(jnp.bfloat16)
        back = lax.dot_general(
            products, back_tab[item], NT, preferred_element_type=jnp.float32
        )
        for start in range(0, block, share):
            column = start * span // LANES * LANES
            joined = jnp.zeros((width, reach), jnp.float32)
            for u in range(start, min(start + share, block)):
                near = back[u * rows : u * rows + width, column : column + reach]
                far = back[u * rows + width : (u + 1) * rows, column : column + reach]
                value = near * sign + far
                keep = across // groups % share == u - start
                joined = value if share == 1 else jnp.where(keep, value, joined)
            total[n, :, column : column + reach] += joined

    def body(step, carry):
        for k in range(UNROLL):
            one(step * UNROLL + k)
        return carry

    lax.fori_loop(0, (ends[-1] + UNROLL - 1) // UNROLL, body, 0)


def return_stage(dims, total, scale, put_refs):
    slots, groups, layers = dims["slots"], dims["groups"], dims["layers"]
    fields, block, count = dims["fields"], dims["block"], 2 * dims["quarter"]
    width, span = fields * 2 * layers, 2 * dims["waves"]
    number = count // block
    share = max(1, LANES // span)
    lane = lax.broadcasted_iota(jnp.int32, (block * groups, POINTS), 1)
    row = lax.broadcasted_iota(jnp.int32, (block * groups, POINTS), 0)
    if span >= LANES:
        owner, kind = lane // span, lane % span // groups
    else:
        owner = lane // LANES * share + lane // groups % share
        kind = lane % LANES // (groups * share)
    pick = (owner * groups + lane % groups == row).astype(jnp.float32).astype(jnp.bfloat16)
    keep = []
    for slot in range(slots):
        for part in range(2):
            at = (kind[:1] == part * slots + slot).astype(jnp.float32)
            keep.append(jnp.broadcast_to(at, (width, POINTS)).astype(jnp.bfloat16))
    for start in range(0, number, 2):
        pieces = []
        for n in range(start, min(start + 2, number)):
            value = total[n] * jnp.concatenate([scale[n]] * fields, 0)
            value = value.astype(jnp.bfloat16)
            pieces += [value * here for here in keep]
        turned = lax.dot_general(
            pick, jnp.concatenate(pieces, 0), NT, preferred_element_type=jnp.float32
        )
        for n in range(start, min(start + 2, number)):
            for u in range(block):
                at = n * block + u
                value = turned[
                    u * groups : (u + 1) * groups, (n - start) * LANES : (n - start + 1) * LANES
                ]
                put_refs[0][pl.ds(at, groups, stride=count), :] = value
                put_refs[1][pl.ds(count - 1 - at, groups, stride=count), :] = value


def grid_scratch(dims):
    slots, groups, block = dims["slots"], dims["groups"], dims["block"]
    layers, fields = dims["layers"], dims["fields"]
    number = 2 * dims["quarter"] // block
    wide = slots * block * groups
    items = -(-most_tiles(dims) // UNROLL) * UNROLL
    width = fields * 2 * layers
    return [
        pltpu.VMEM((2, wide, LANES), jnp.float32),
        pltpu.VMEM((2, wide, LANES), jnp.float32),
        pltpu.VMEM((items, 2 * wide, POINTS), jnp.bfloat16),
        pltpu.VMEM((items, 2 * wide, POINTS), jnp.bfloat16),
        pltpu.VMEM((number + 1, block * 2 * layers, LANES), jnp.float32),
        pltpu.VMEM((number, 2 * layers, POINTS), jnp.float32),
        pltpu.VMEM((number + 1, width, 2 * wide), jnp.bfloat16),
        pltpu.VMEM((number + 1, width, 2 * wide), jnp.float32),
    ]


def final_stage(dims, get, leg_ref, perm_ref):
    slots, columns, half = dims["slots"], dims["columns"], dims["half"]
    turned = lax.dot_general(
        perm_ref[...], get, NT, preferred_element_type=jnp.float32
    ).astype(jnp.bfloat16)
    results = []
    for slot in range(slots):
        total = 0.0
        for hemi in range(2):
            at = (slot * 2 + hemi) * columns
            total += jnp.dot(
                turned[at : at + columns],
                leg_ref[slot, hemi * half : (hemi + 1) * half, :],
                preferred_element_type=jnp.float32,
            )
        results.append(total)
    return results


def joined_rows(dims, back_ref):
    quarter, groups = dims["quarter"], dims["groups"]
    low = [back_ref[place][:quarter] for place in range(groups)]
    high = [back_ref[place][quarter:] for place in reversed(range(groups))]
    return low + high


def to_peer(axis, shift):
    place = lax.axis_index(axis)
    count = lax.axis_size(axis)
    return {axis: lax.rem(place + shift, count)}


def exchange(axis, source_of, target_of, sems):
    place = lax.axis_index(axis)
    count = lax.axis_size(axis)
    copies = []
    for shift in range(1, count):
        peer = lax.rem(place + shift, count)
        copies.append(
            pltpu.make_async_remote_copy(
                src_ref=source_of(peer),
                dst_ref=target_of(place),
                send_sem=sems[0].at[shift],
                recv_sem=sems[1].at[shift],
                device_id=to_peer(axis, shift),
                device_id_type=pl.DeviceIdType.MESH,
            )
        )
    return copies


def whole_kernel(
    dims, spec_ref, leg_hbm, perm_ref, share_ref, quad_ref, cor_ref, wave_ref, out_ref,
    leg, rows, send, recv, back_send, back, wave_send, wave_recv, sum_send, sum_recv, geo,
    get, north, south, load_sem, sem_a, sem_b, sem_c, sem_d, sem_e, sem_f, sem_g, sem_h, *scratch,
):
    slots, groups, half = dims["slots"], dims["groups"], dims["half"]
    fields, layers, count = dims["fields"], dims["layers"], 2 * dims["quarter"]
    degrees = spec_ref.shape[2]
    me = lax.axis_index("wave")
    floor = lax.axis_index("lev")
    floors = lax.axis_size("lev")
    loads = []
    for slot in range(slots):
        for hemi in range(2):
            piece = pl.ds(hemi * half, half)
            copy = pltpu.make_async_copy(
                leg_hbm.at[slot, piece], leg.at[slot, piece], load_sem.at[slot * 2 + hemi]
            )
            copy.start()
            loads.append(copy)
    barrier = pltpu.get_barrier_semaphore()
    for axis, size in (("wave", groups), ("lev", floors)):
        for shift in range(1, size):
            pl.semaphore_signal(
                barrier, inc=1, device_id=to_peer(axis, shift), device_id_type=pl.DeviceIdType.MESH
            )
    degree = lax.broadcasted_iota(jnp.int32, (1, degrees), 1)
    live = [
        jnp.where(degree < degrees - wave_ref[slot], 1.0, 0.0).astype(jnp.float32)
        for slot in range(slots)
    ]
    row = lax.broadcasted_iota(jnp.int32, (8, LANES), 0)
    own = jnp.zeros((8, LANES), jnp.float32)
    for slot in range(slots):
        own = jnp.where(row == slot, wave_ref[slot].astype(jnp.float32), own)
    wave_send[...] = own
    geo[...] = jnp.zeros_like(geo)
    for slot in range(slots):
        full = spec_ref[slot].astype(jnp.float32) * live[slot]
        for part in range(2):
            first = part * fields * layers
            total = jnp.zeros((1, degrees), jnp.float32)
            for layer in reversed(range(layers)):
                at = first + 3 * layers + layer
                total = total + full[at : at + 1] * share_ref[layer]
                at = first + 2 * layers + layer
                geo[slot, at : at + 1, :] = total
            at = slot * 2 + part
            sum_send[at : at + 1, :] = total
    place = lax.broadcasted_iota(jnp.int32, (1, LANES), 1) // (LANES // slots)
    gain = jnp.ones((1, LANES), jnp.float32)
    for slot in range(slots):
        twice = jnp.where(wave_ref[slot] == 0, 1.0, 2.0)
        gain = jnp.where(place == slot, twice, gain)
    fourier_stage(dims, spec_ref, leg, loads, live, gain, perm_ref, rows)
    split_rows(dims, rows, send)
    pl.semaphore_wait(barrier, groups - 1 + floors - 1)

    def wave_place(device):
        return wave_recv.at[pl.ds(pl.multiple_of(device * 8, 8), 8)]

    tell = exchange("wave", lambda _: wave_send, wave_place, (sem_a, sem_b))
    lift = exchange("lev", lambda _: sum_send, lambda p: sum_recv.at[p], (sem_c, sem_d))
    for copy in tell:
        copy.start()
    wave_recv[pl.ds(pl.multiple_of(me * 8, 8), 8), :] = own
    there = exchange("wave", lambda p: send.at[p], lambda p: recv.at[p], (sem_e, sem_f))
    for copy in there + lift:
        copy.start()
    recv[me] = send[me]
    for copy in tell:
        copy.wait()
    waves = [wave_recv[pl.ds(slot, groups, stride=8), :] for slot in range(slots)]
    state, hop, tab, back_tab, cor, scale, base, total = scratch
    table_stage(dims, me, waves, quad_ref, cor_ref, scratch[:6])
    for copy in there:
        copy.wait()
    for source in range(groups):
        get[source * count : (source + 1) * count, :] = recv[source].astype(jnp.float32)
    coefficient_stage(dims, get, base, total)
    item_stage(dims, me, base, tab, back_tab, cor, total)
    return_stage(dims, total, scale, (north, south))
    hemi = lax.broadcasted_iota(jnp.int32, (count, LANES), 1) // layers % 2
    for source in range(groups):
        piece = slice(source * count, (source + 1) * count)
        back_send[source] = jnp.where(hemi == 1, south[piece], north[piece]).astype(jnp.bfloat16)
    home = exchange("wave", lambda p: back_send.at[p], lambda p: back.at[p], (sem_g, sem_h))
    for copy in home:
        copy.start()
    back[me] = back_send[me]
    for copy in lift:
        copy.wait()
    for slot in range(slots):
        for part in range(2):
            at = slot * 2 + part
            deeper = jnp.zeros((1, degrees), jnp.float32)
            for other in range(floors):
                value = sum_recv[other, at : at + 1, :]
                deeper = deeper + jnp.where(other > floor, value, 0.0)
            first = (part * fields + 2) * layers
            geo[slot, first : first + layers, :] += deeper
    for copy in home:
        copy.wait()
    pieces = [piece.astype(jnp.float32) for piece in joined_rows(dims, back)]
    joined = jnp.concatenate(pieces, 0).astype(jnp.bfloat16)
    for slot, value in enumerate(final_stage(dims, joined, leg, perm_ref)):
        out_ref[slot] = ((value + geo[slot]) * live[slot]).astype(jnp.bfloat16)


def body(spec, legendre, layer_depth_share, quad_weight, wave_of_slot):
    slots, columns, degrees = spec.shape
    total_lat = legendre.shape[1]
    groups = lax.axis_size("wave")
    layers = layer_depth_share.shape[0]
    quarter = total_lat // groups // 4
    depth = 2 * slots * groups
    block = max(b for b in range(1, quarter + 1) if quarter % b == 0 and b * depth <= max(256, depth))
    dims = dict(
        slots=slots, columns=columns, half=total_lat // 2, groups=groups, layers=layers,
        fields=columns // (2 * layers), quarter=quarter, block=block, waves=slots * groups,
    )
    fields = dims["fields"]
    maps = lane_maps(slots, fields, layers)
    perm = np.zeros((LANES, LANES), np.float32)
    perm[maps, np.arange(LANES)] = 1.0
    perm = jnp.asarray(perm, jnp.bfloat16)
    lat = np.arange(total_lat)
    coriolis = jnp.asarray(2.0 * np.cos(np.pi * (lat + 0.5) / total_lat), jnp.float32)
    floors = lax.axis_size("lev")
    half, count = total_lat // 2, 2 * quarter
    vmem = pl.BlockSpec(memory_space=pltpu.VMEM)
    smem = pl.BlockSpec(memory_space=pltpu.SMEM)
    rows = pltpu.VMEM((groups, count, LANES), jnp.bfloat16)
    flat = pltpu.VMEM((groups * count, LANES), jnp.float32)
    sums = 2 * slots
    return pl.pallas_call(
        functools.partial(whole_kernel, dims),
        out_shape=jax.ShapeDtypeStruct(spec.shape, jnp.bfloat16),
        in_specs=[vmem, pl.BlockSpec(memory_space=pl.ANY), vmem] + [smem] * 4,
        out_specs=vmem,
        scratch_shapes=[
            pltpu.VMEM(legendre.shape, jnp.bfloat16),
            pltpu.VMEM((half, LANES), jnp.float32),
            rows, rows, rows, rows,
            pltpu.VMEM((8, LANES), jnp.float32),
            pltpu.VMEM((groups * 8, LANES), jnp.float32),
            pltpu.VMEM((sums, degrees), jnp.float32),
            pltpu.VMEM((floors, sums, degrees), jnp.float32),
            pltpu.VMEM(spec.shape, jnp.float32),
            flat, flat, flat,
            pltpu.SemaphoreType.DMA((2 * slots,)),
            pltpu.SemaphoreType.DMA((groups,)),
            pltpu.SemaphoreType.DMA((groups,)),
            pltpu.SemaphoreType.DMA((floors,)),
            pltpu.SemaphoreType.DMA((floors,)),
            pltpu.SemaphoreType.DMA((groups,)),
            pltpu.SemaphoreType.DMA((groups,)),
            pltpu.SemaphoreType.DMA((groups,)),
            pltpu.SemaphoreType.DMA((groups,)),
        ]
        + grid_scratch(dims),
        compiler_params=pltpu.CompilerParams(collective_id=0, has_side_effects=True),
    )(spec, legendre, perm, layer_depth_share, quad_weight, coriolis, wave_of_slot)


def solution(mesh):
    in_specs = (P("wave", "lev", None), P("wave", None, None), P("lev"), P(), P("wave"))
    out_specs = P("wave", "lev", None)
    return jax.shard_map(body, mesh=mesh, in_specs=in_specs, out_specs=out_specs, check_vma=False)
```

```python
import functools
import math

import jax
import jax.numpy as jnp
import numpy as np
from jax import lax
from jax.experimental import pallas as pl
from jax.experimental.pallas import tpu as pltpu
from jax.sharding import PartitionSpec as P

LANES = 128
POINTS = 2 * LANES
UNROLL = 16
VMEM_BYTES = 48 * 2**20
NT = (((1,), (1,)), ((), ()))


def taylor(first, count):
    return [(-1.0) ** k / math.factorial(2 * k + first) for k in range(count)]


def horner(square, terms):
    total = jnp.full_like(square, terms[-1])
    for term in reversed(terms[:-1]):
        total = total * square + term
    return total


def turn_trig(steps, length, inverse):
    whole = jnp.floor(steps * inverse + 0.5)
    angle = (steps - whole * length) * inverse * (2.0 * math.pi)
    square = angle * angle
    return horner(square, taylor(0, 10)), angle * horner(square, taylor(1, 10))


def lane_maps(slots, fields, layers):
    order = np.arange(slots * 2 * 2 * fields * layers)
    natural = order.reshape(slots, 2, 2, fields, layers)
    return natural.transpose(0, 2, 3, 1, 4).reshape(-1)


def fourier_stage(dims, spec_ref, leg_ref, loads, live, gain, perm_ref, rows_ref):
    slots, columns, half = dims["slots"], dims["columns"], dims["half"]
    total = jnp.zeros((half, LANES), jnp.float32)
    for slot in range(slots):
        masked = spec_ref[slot] * live[slot].astype(jnp.bfloat16)
        for hemi in range(2):
            at = (slot * 2 + hemi) * columns
            pieces = []
            if at:
                pieces.append(jnp.zeros((at, masked.shape[1]), masked.dtype))
            pieces.append(masked)
            if at + columns < LANES:
                pieces.append(jnp.zeros((LANES - at - columns, masked.shape[1]), masked.dtype))
            loads[slot * 2 + hemi].wait()
            total += lax.dot_general(
                leg_ref[slot, hemi * half : (hemi + 1) * half, :],
                jnp.concatenate(pieces, 0),
                NT,
                preferred_element_type=jnp.float32,
            )
    rows = jnp.dot(total.astype(jnp.bfloat16), perm_ref[...], preferred_element_type=jnp.float32)
    rows_ref[...] = rows * gain


def split_rows(dims, rows_ref, send_ref):
    quarter, half = dims["quarter"], dims["half"]
    for place in range(dims["groups"]):
        low = rows_ref[place * quarter : (place + 1) * quarter, :]
        top = half - place * quarter
        high = rows_ref[top - quarter : top, :]
        send_ref[place] = jnp.concatenate([low, high], 0).astype(jnp.bfloat16)


def whereabouts(dims, device, number):
    quarter, block = dims["quarter"], dims["block"]
    local = [number * block + u for u in range(block)]
    dist = [
        jnp.where(
            r < quarter, device * quarter + r, dims["half"] - (device + 2) * quarter + r
        )
        for r in local
    ]
    lengths = [20 + 4 * q for q in dist]
    return local, dist, lengths, [length.astype(jnp.float32) for length in lengths]


def tiles_of(longest):
    return (longest // 2 + POINTS) // POINTS


def most_tiles(dims):
    quarter, block, half = dims["quarter"], dims["block"], dims["half"]
    most = 0
    for device in range(dims["groups"]):
        total = 0
        for number in range(2 * quarter // block):
            r = number * block + block - 1
            q = device * quarter + r if r < quarter else half - (device + 2) * quarter + r
            total += tiles_of(20 + 4 * q)
        most = max(most, total)
    return most


def back_home(dims, part, slot, u):
    width = 2 * dims["waves"]
    if width >= LANES:
        return u * width + part * dims["waves"] + slot * dims["groups"]
    share = LANES // width
    inner = (part * dims["slots"] + slot) * share + u % share
    return u // share * LANES + inner * dims["groups"]


def table_stage(dims, device, waves, quad_ref, cor_ref, scratch):
    slots, groups, half = dims["slots"], dims["groups"], dims["half"]
    fields, layers, block = dims["fields"], dims["layers"], dims["block"]
    state, hop, tab, back_tab, cor, scale = scratch
    total_lat = 2 * half
    pair = min(2, block)
    wide = slots * block * groups
    lane = lax.broadcasted_iota(jnp.int32, (groups, LANES), 1).astype(jnp.float32)
    north_row = lax.broadcasted_iota(jnp.int32, (2 * layers, LANES), 0) < layers
    wave_row = lax.broadcasted_iota(jnp.int32, (2 * layers, POINTS), 0) < layers
    width = 2 * dims["waves"]
    column = lax.broadcasted_iota(jnp.int32, (2 * layers, POINTS), 1)
    if width >= LANES:
        owner = column // width
    else:
        share = LANES // width
        owner = column // LANES * share + column // groups % share

    def group(number, first):
        local, dist, lengths, floats = whereabouts(dims, device, number)
        scaled = jnp.zeros((2 * layers, POINTS), jnp.float32)
        for u, length in enumerate(floats):
            inverse = 1.0 / jnp.full((groups, LANES), length, jnp.float32)
            for slot in range(slots):
                begin = turn_trig(waves[slot] * lane, length, inverse)
                cosine = jnp.broadcast_to(begin[0][:, LANES // 2 : LANES // 2 + 1], (groups, LANES))
                sine = jnp.broadcast_to(begin[1][:, LANES // 2 : LANES // 2 + 1], (groups, LANES))
                keep = jnp.where(2.0 * waves[slot] < length, 1.0, 0.0)
                at = (slot * block + u) * groups
                state[0, at : at + groups, :] = begin[0] * keep
                state[1, at : at + groups, :] = begin[1] * keep
                hop[0, at : at + groups, :] = cosine * cosine - sine * sine
                hop[1, at : at + groups, :] = 2.0 * cosine * sine
            cor[number, u * 2 * layers : (u + 1) * 2 * layers, :] = jnp.where(
                north_row, cor_ref[dist[u]], cor_ref[total_lat - 1 - dist[u]]
            )
            here = jnp.where(wave_row, quad_ref[dist[u]], quad_ref[total_lat - 1 - dist[u]])
            scaled = jnp.where(owner == u, here / length, scaled)
        scale[number] = scaled

        def tile(index, item):
            for side in range(POINTS // LANES):
                cols = slice(side * LANES, (side + 1) * LANES)
                point = lane + (index * POINTS + side * LANES).astype(jnp.float32)
                start = jnp.minimum(point + 0.5, 1.0)
                weight = [
                    jnp.maximum(jnp.minimum(0.5 * length + 0.5 - point, start), 0.0)
                    for length in floats
                ]
                for u in range(0, block, pair):
                    both = jnp.concatenate(weight[u : u + pair], 0).astype(jnp.bfloat16)
                    for slot in range(slots):
                        at = (slot * block + u) * groups
                        rows = slice(at, at + pair * groups)
                        cosine, sine = state[0, rows, :], state[1, rows, :]
                        turn_cos, turn_sin = hop[0, rows, :], hop[1, rows, :]
                        state[0, rows, :] = cosine * turn_cos - sine * turn_sin
                        state[1, rows, :] = sine * turn_cos + cosine * turn_sin
                        for part, value in enumerate((cosine, sine)):
                            packed = value.astype(jnp.bfloat16)
                            put = part * wide + at
                            tab[item, put : put + pair * groups, cols] = packed
                            put = back_home(dims, part, slot, u)
                            back_tab[item, put : put + pair * groups, cols] = packed * both
            return item + 1

        return lax.fori_loop(0, tiles_of(lengths[-1]), tile, first)

    lax.fori_loop(0, 2 * dims["quarter"] // block, group, 0)


def coefficient_stage(dims, get_ref, base, total):
    slots, groups, layers = dims["slots"], dims["groups"], dims["layers"]
    fields, block, count = dims["fields"], dims["block"], 2 * dims["quarter"]
    width = fields * 2 * layers
    number = count // block
    lane = lax.broadcasted_iota(jnp.int32, (groups, LANES), 1)
    south_lane = lane // layers % 2 == 1
    first_slot = lax.broadcasted_iota(jnp.int32, (width, LANES), 1) < block * groups
    eye = (
        lax.broadcasted_iota(jnp.int32, (LANES, LANES), 0)
        == lax.broadcasted_iota(jnp.int32, (LANES, LANES), 1)
    ).astype(jnp.bfloat16)
    for start in range(0, number, 2):
        pieces = []
        for n in range(start, min(start + 2, number)):
            both = []
            for u in range(block):
                at = n * block + u
                north = get_ref[pl.ds(at, groups, stride=count), :]
                south = get_ref[pl.ds(count - 1 - at, groups, stride=count), :]
                both.append(jnp.where(south_lane, south, north))
            pieces += both * (LANES // (block * groups))
        turned = lax.dot_general(
            eye,
            jnp.concatenate(pieces, 0).astype(jnp.bfloat16),
            NT,
            preferred_element_type=jnp.float32,
        )
        for n in range(start, min(start + 2, number)):
            mine = turned[:, (n - start) * LANES : (n - start + 1) * LANES]
            for part in range(2):
                value = [
                    mine[(slot * 2 + part) * width : (slot * 2 + part + 1) * width]
                    for slot in range(slots)
                ]
                base[n, :, part * LANES : (part + 1) * LANES] = jnp.where(
                    first_slot, value[0], value[1]
                ).astype(jnp.bfloat16)
    total[...] = jnp.zeros_like(total)


def item_stage(dims, device, base, tab, back_tab, cor, total):
    groups, layers, block = dims["groups"], dims["layers"], dims["block"]
    fields, number = dims["fields"], 2 * dims["quarter"] // dims["block"]
    width = fields * 2 * layers
    rows = 2 * width
    ends = []
    for n in range(number):
        lengths = whereabouts(dims, device, n)[2]
        ends.append(tiles_of(lengths[-1]) + (ends[-1] if ends else 0))
    lane = lax.broadcasted_iota(jnp.int32, (width, LANES), 1)
    mine = [
        (lane // groups % block == u).astype(jnp.float32).astype(jnp.bfloat16)
        for u in range(block)
    ]
    span = 2 * dims["waves"]
    share = max(1, LANES // span)
    reach = max(LANES, span)
    across = lax.broadcasted_iota(jnp.int32, (width, reach), 1)
    sign = jnp.where(across // (reach // 2) == 0, 1.0, -1.0)

    def one(item):
        n = 0
        for end in ends:
            n = n + jnp.where(item >= end, 1, 0)
        real = base[n, :, :LANES]
        imag = base[n, :, LANES:]
        pieces = []
        for u in range(block):
            left, right = real * mine[u], imag * mine[u]
            pieces.append(jnp.concatenate([left, -right], 1))
            pieces.append(jnp.concatenate([left, right], 1))
        grid = jnp.dot(
            jnp.concatenate(pieces, 0), tab[item], preferred_element_type=jnp.float32
        )
        made = []
        for u in range(block):
            extra = cor[n, u * 2 * layers : (u + 1) * 2 * layers, :]
            extra = jnp.concatenate([extra] * (POINTS // LANES), 1)
            for side in range(2):
                at = (u * 2 + side) * width
                part = [
                    grid[at + f * 2 * layers : at + (f + 1) * 2 * layers] for f in range(fields)
                ]
                absolute = part[2] + extra
                made += [
                    absolute * part[0],
                    absolute * part[1],
                    0.5 * (part[0] * part[0] + part[1] * part[1]),
                    part[0] * part[3],
                ]
        products = jnp.concatenate(made, 0).astype(jnp.bfloat16)
        back = lax.dot_general(
            products, back_tab[item], NT, preferred_element_type=jnp.float32
        )
        for start in range(0, block, share):
            column = start * span // LANES * LANES
            joined = jnp.zeros((width, reach), jnp.float32)
            for u in range(start, min(start + share, block)):
                near = back[u * rows : u * rows + width, column : column + reach]
                far = back[u * rows + width : (u + 1) * rows, column : column + reach]
                value = near * sign + far
                keep = across // groups % share == u - start
                joined = value if share == 1 else jnp.where(keep, value, joined)
            total[n, :, column : column + reach] += joined

    def body(step, carry):
        for k in range(UNROLL):
            one(step * UNROLL + k)
        return carry

    lax.fori_loop(0, (ends[-1] + UNROLL - 1) // UNROLL, body, 0)


def return_stage(dims, total, scale, put_refs):
    slots, groups, layers = dims["slots"], dims["groups"], dims["layers"]
    fields, block, count = dims["fields"], dims["block"], 2 * dims["quarter"]
    width, span = fields * 2 * layers, 2 * dims["waves"]
    number = count // block
    share = max(1, LANES // span)
    lane = lax.broadcasted_iota(jnp.int32, (block * groups, POINTS), 1)
    row = lax.broadcasted_iota(jnp.int32, (block * groups, POINTS), 0)
    if span >= LANES:
        owner, kind = lane // span, lane % span // groups
    else:
        owner = lane // LANES * share + lane // groups % share
        kind = lane % LANES // (groups * share)
    pick = (owner * groups + lane % groups == row).astype(jnp.float32).astype(jnp.bfloat16)
    keep = []
    for slot in range(slots):
        for part in range(2):
            at = (kind[:1] == part * slots + slot).astype(jnp.float32)
            keep.append(jnp.broadcast_to(at, (width, POINTS)).astype(jnp.bfloat16))
    for start in range(0, number, 2):
        pieces = []
        for n in range(start, min(start + 2, number)):
            value = total[n] * jnp.concatenate([scale[n]] * fields, 0)
            value = value.astype(jnp.bfloat16)
            pieces += [value * here for here in keep]
        turned = lax.dot_general(
            pick, jnp.concatenate(pieces, 0), NT, preferred_element_type=jnp.float32
        )
        for n in range(start, min(start + 2, number)):
            for u in range(block):
                at = n * block + u
                value = turned[
                    u * groups : (u + 1) * groups, (n - start) * LANES : (n - start + 1) * LANES
                ]
                put_refs[0][pl.ds(at, groups, stride=count), :] = value
                put_refs[1][pl.ds(count - 1 - at, groups, stride=count), :] = value


def grid_scratch(dims):
    slots, groups, block = dims["slots"], dims["groups"], dims["block"]
    layers, fields = dims["layers"], dims["fields"]
    number = 2 * dims["quarter"] // block
    wide = slots * block * groups
    items = -(-most_tiles(dims) // UNROLL) * UNROLL
    width = fields * 2 * layers
    return [
        pltpu.VMEM((2, wide, LANES), jnp.float32),
        pltpu.VMEM((2, wide, LANES), jnp.float32),
        pltpu.VMEM((items, 2 * wide, POINTS), jnp.bfloat16),
        pltpu.VMEM((items, 2 * wide, POINTS), jnp.bfloat16),
        pltpu.VMEM((number + 1, block * 2 * layers, LANES), jnp.float32),
        pltpu.VMEM((number, 2 * layers, POINTS), jnp.float32),
        pltpu.VMEM((number + 1, width, 2 * wide), jnp.bfloat16),
        pltpu.VMEM((number + 1, width, 2 * wide), jnp.float32),
    ]


def final_stage(dims, get, leg_ref, perm_ref):
    slots, columns, half = dims["slots"], dims["columns"], dims["half"]
    turned = lax.dot_general(
        perm_ref[...], get, NT, preferred_element_type=jnp.float32
    ).astype(jnp.bfloat16)
    results = []
    for slot in range(slots):
        total = 0.0
        for hemi in range(2):
            at = (slot * 2 + hemi) * columns
            total += jnp.dot(
                turned[at : at + columns],
                leg_ref[slot, hemi * half : (hemi + 1) * half, :],
                preferred_element_type=jnp.float32,
            )
        results.append(total)
    return results


def joined_rows(dims, back_ref):
    quarter, groups = dims["quarter"], dims["groups"]
    low = [back_ref[place][:quarter] for place in range(groups)]
    high = [back_ref[place][quarter:] for place in reversed(range(groups))]
    return low + high


def to_peer(axis, shift):
    place = lax.axis_index(axis)
    count = lax.axis_size(axis)
    return {axis: lax.rem(place + shift, count)}


def exchange(axis, source_of, target_of, sems):
    place = lax.axis_index(axis)
    count = lax.axis_size(axis)
    copies = []
    for shift in range(1, count):
        peer = lax.rem(place + shift, count)
        copies.append(
            pltpu.make_async_remote_copy(
                src_ref=source_of(peer),
                dst_ref=target_of(place),
                send_sem=sems[0].at[shift],
                recv_sem=sems[1].at[shift],
                device_id=to_peer(axis, shift),
                device_id_type=pl.DeviceIdType.MESH,
            )
        )
    return copies


def whole_kernel(
    dims, spec_hbm, leg_hbm, perm_hbm, share_hbm, quad_hbm, cor_hbm, wave_hbm, out_ref,
    spec_ref, perm_ref, share_ref, quad_ref, cor_ref, wave_ref, in_sem,
    leg, rows, send, recv, back_send, back, wave_send, wave_recv, sum_send, sum_recv, geo,
    get, north, south, load_sem, sem_a, sem_b, sem_c, sem_d, sem_e, sem_f, sem_g, sem_h, *scratch,
):
    slots, groups, half = dims["slots"], dims["groups"], dims["half"]
    fields, layers, count = dims["fields"], dims["layers"], 2 * dims["quarter"]
    degrees = spec_hbm.shape[2]
    me = lax.axis_index("wave")
    floor = lax.axis_index("lev")
    floors = lax.axis_size("lev")
    pairs = (
        (spec_hbm, spec_ref), (wave_hbm, wave_ref), (share_hbm, share_ref),
        (perm_hbm, perm_ref), (quad_hbm, quad_ref), (cor_hbm, cor_ref),
    )
    brought = [
        pltpu.make_async_copy(source, target, in_sem.at[k])
        for k, (source, target) in enumerate(pairs)
    ]
    for copy in brought:
        copy.start()
    loads = []
    for slot in range(slots):
        for hemi in range(2):
            piece = pl.ds(hemi * half, half)
            copy = pltpu.make_async_copy(
                leg_hbm.at[slot, piece], leg.at[slot, piece], load_sem.at[slot * 2 + hemi]
            )
            copy.start()
            loads.append(copy)
    barrier = pltpu.get_barrier_semaphore()
    for axis, size in (("wave", groups), ("lev", floors)):
        for shift in range(1, size):
            pl.semaphore_signal(
                barrier, inc=1, device_id=to_peer(axis, shift), device_id_type=pl.DeviceIdType.MESH
            )
    for copy in brought:
        copy.wait()
    degree = lax.broadcasted_iota(jnp.int32, (1, degrees), 1)
    live = [
        jnp.where(degree < degrees - wave_ref[slot], 1.0, 0.0).astype(jnp.float32)
        for slot in range(slots)
    ]
    row = lax.broadcasted_iota(jnp.int32, (8, LANES), 0)
    own = jnp.zeros((8, LANES), jnp.float32)
    for slot in range(slots):
        own = jnp.where(row == slot, wave_ref[slot].astype(jnp.float32), own)
    wave_send[...] = own
    geo[...] = jnp.zeros_like(geo)
    for slot in range(slots):
        full = spec_ref[slot].astype(jnp.float32) * live[slot]
        for part in range(2):
            first = part * fields * layers
            total = jnp.zeros((1, degrees), jnp.float32)
            for layer in reversed(range(layers)):
                at = first + 3 * layers + layer
                total = total + full[at : at + 1] * share_ref[layer]
                at = first + 2 * layers + layer
                geo[slot, at : at + 1, :] = total
            at = slot * 2 + part
            sum_send[at : at + 1, :] = total
    place = lax.broadcasted_iota(jnp.int32, (1, LANES), 1) // (LANES // slots)
    gain = jnp.ones((1, LANES), jnp.float32)
    for slot in range(slots):
        twice = jnp.where(wave_ref[slot] == 0, 1.0, 2.0)
        gain = jnp.where(place == slot, twice, gain)
    fourier_stage(dims, spec_ref, leg, loads, live, gain, perm_ref, rows)
    split_rows(dims, rows, send)
    pl.semaphore_wait(barrier, groups - 1 + floors - 1)

    def wave_place(device):
        return wave_recv.at[pl.ds(pl.multiple_of(device * 8, 8), 8)]

    tell = exchange("wave", lambda _: wave_send, wave_place, (sem_a, sem_b))
    lift = exchange("lev", lambda _: sum_send, lambda p: sum_recv.at[p], (sem_c, sem_d))
    for copy in tell:
        copy.start()
    wave_recv[pl.ds(pl.multiple_of(me * 8, 8), 8), :] = own
    there = exchange("wave", lambda p: send.at[p], lambda p: recv.at[p], (sem_e, sem_f))
    for copy in there + lift:
        copy.start()
    recv[me] = send[me]
    for copy in tell:
        copy.wait()
    waves = [wave_recv[pl.ds(slot, groups, stride=8), :] for slot in range(slots)]
    state, hop, tab, back_tab, cor, scale, base, total = scratch
    table_stage(dims, me, waves, quad_ref, cor_ref, scratch[:6])
    for copy in there:
        copy.wait()
    for source in range(groups):
        get[source * count : (source + 1) * count, :] = recv[source].astype(jnp.float32)
    coefficient_stage(dims, get, base, total)
    item_stage(dims, me, base, tab, back_tab, cor, total)
    return_stage(dims, total, scale, (north, south))
    hemi = lax.broadcasted_iota(jnp.int32, (count, LANES), 1) // layers % 2
    for source in range(groups):
        piece = slice(source * count, (source + 1) * count)
        back_send[source] = jnp.where(hemi == 1, south[piece], north[piece]).astype(jnp.bfloat16)
    home = exchange("wave", lambda p: back_send.at[p], lambda p: back.at[p], (sem_g, sem_h))
    for copy in home:
        copy.start()
    back[me] = back_send[me]
    for copy in lift:
        copy.wait()
    for slot in range(slots):
        for part in range(2):
            at = slot * 2 + part
            deeper = jnp.zeros((1, degrees), jnp.float32)
            for other in range(floors):
                value = sum_recv[other, at : at + 1, :]
                deeper = deeper + jnp.where(other > floor, value, 0.0)
            first = (part * fields + 2) * layers
            geo[slot, first : first + layers, :] += deeper
    for copy in home:
        copy.wait()
    pieces = [piece.astype(jnp.float32) for piece in joined_rows(dims, back)]
    joined = jnp.concatenate(pieces, 0).astype(jnp.bfloat16)
    for slot, value in enumerate(final_stage(dims, joined, leg, perm_ref)):
        out_ref[slot] = ((value + geo[slot]) * live[slot]).astype(jnp.bfloat16)


def body(spec, legendre, layer_depth_share, quad_weight, wave_of_slot):
    slots, columns, degrees = spec.shape
    total_lat = legendre.shape[1]
    groups = lax.axis_size("wave")
    layers = layer_depth_share.shape[0]
    quarter = total_lat // groups // 4
    depth = 2 * slots * groups
    block = max(b for b in range(1, quarter + 1) if quarter % b == 0 and b * depth <= max(256, depth))
    dims = dict(
        slots=slots, columns=columns, half=total_lat // 2, groups=groups, layers=layers,
        fields=columns // (2 * layers), quarter=quarter, block=block, waves=slots * groups,
    )
    fields = dims["fields"]
    maps = lane_maps(slots, fields, layers)
    perm = np.zeros((LANES, LANES), np.float32)
    perm[maps, np.arange(LANES)] = 1.0
    perm = jnp.asarray(perm, jnp.bfloat16)
    lat = np.arange(total_lat)
    coriolis = jnp.asarray(2.0 * np.cos(np.pi * (lat + 0.5) / total_lat), jnp.float32)
    floors = lax.axis_size("lev")
    half, count = total_lat // 2, 2 * quarter
    vmem = pl.BlockSpec(memory_space=pltpu.VMEM)
    rows = pltpu.VMEM((groups, count, LANES), jnp.bfloat16)
    flat = pltpu.VMEM((groups * count, LANES), jnp.float32)
    sums = 2 * slots
    operands = (spec, legendre, perm, layer_depth_share, quad_weight, coriolis, wave_of_slot)
    operands = [pltpu.with_memory_space_constraint(x, pltpu.HBM) for x in operands]
    return pl.pallas_call(
        functools.partial(whole_kernel, dims),
        out_shape=jax.ShapeDtypeStruct(spec.shape, jnp.bfloat16),
        in_specs=[pl.BlockSpec(memory_space=pltpu.HBM)] * len(operands),
        out_specs=vmem,
        scratch_shapes=[
            pltpu.VMEM(spec.shape, jnp.bfloat16),
            pltpu.VMEM((LANES, LANES), jnp.bfloat16),
            pltpu.SMEM(layer_depth_share.shape, jnp.float32),
            pltpu.SMEM(quad_weight.shape, jnp.float32),
            pltpu.SMEM(quad_weight.shape, jnp.float32),
            pltpu.SMEM(wave_of_slot.shape, jnp.int32),
            pltpu.SemaphoreType.DMA((6,)),
            pltpu.VMEM(legendre.shape, jnp.bfloat16),
            pltpu.VMEM((half, LANES), jnp.float32),
            rows, rows, rows, rows,
            pltpu.VMEM((8, LANES), jnp.float32),
            pltpu.VMEM((groups * 8, LANES), jnp.float32),
            pltpu.VMEM((sums, degrees), jnp.float32),
            pltpu.VMEM((floors, sums, degrees), jnp.float32),
            pltpu.VMEM(spec.shape, jnp.float32),
            flat, flat, flat,
            pltpu.SemaphoreType.DMA((2 * slots,)),
            pltpu.SemaphoreType.DMA((groups,)),
            pltpu.SemaphoreType.DMA((groups,)),
            pltpu.SemaphoreType.DMA((floors,)),
            pltpu.SemaphoreType.DMA((floors,)),
            pltpu.SemaphoreType.DMA((groups,)),
            pltpu.SemaphoreType.DMA((groups,)),
            pltpu.SemaphoreType.DMA((groups,)),
            pltpu.SemaphoreType.DMA((groups,)),
        ]
        + grid_scratch(dims),
        compiler_params=pltpu.CompilerParams(collective_id=0, has_side_effects=True, vmem_limit_bytes=VMEM_BYTES),
    )(*operands)


def solution(mesh):
    in_specs = (P("wave", "lev", None), P("wave", None, None), P("lev"), P(), P("wave"))
    out_specs = P("wave", "lev", None)
    return jax.shard_map(body, mesh=mesh, in_specs=in_specs, out_specs=out_specs, check_vma=False)
```

```python
import functools
import math

import jax
import jax.numpy as jnp
import numpy as np
from jax import lax
from jax.experimental import pallas as pl
from jax.experimental.pallas import tpu as pltpu
from jax.sharding import PartitionSpec as P

LANES = 128
POINTS = 2 * LANES
UNROLL = 16
FILLS = 4
VMEM_BYTES = 48 * 2**20
NT = (((1,), (1,)), ((), ()))


def taylor(first, count):
    return [(-1.0) ** k / math.factorial(2 * k + first) for k in range(count)]


def horner(square, terms):
    total = jnp.full_like(square, terms[-1])
    for term in reversed(terms[:-1]):
        total = total * square + term
    return total


def turn_trig(steps, length, inverse):
    whole = jnp.floor(steps * inverse + 0.5)
    angle = (steps - whole * length) * (inverse * math.pi)
    square = angle * angle
    sine = angle * horner(square, taylor(1, 6))
    twice = sine + sine
    return 1.0 - twice * sine, twice * horner(square, taylor(0, 7))


def lane_maps(slots, fields, layers):
    order = np.arange(slots * 2 * 2 * fields * layers)
    natural = order.reshape(slots, 2, 2, fields, layers)
    return natural.transpose(0, 2, 3, 1, 4).reshape(-1)


def fourier_stage(dims, spec_ref, leg_ref, loads, live, gain, perm_ref, rows_ref):
    slots, columns, half = dims["slots"], dims["columns"], dims["half"]
    total = jnp.zeros((half, LANES), jnp.float32)
    for slot in range(slots):
        masked = spec_ref[slot] * live[slot].astype(jnp.bfloat16)
        for hemi in range(2):
            at = (slot * 2 + hemi) * columns
            pieces = []
            if at:
                pieces.append(jnp.zeros((at, masked.shape[1]), masked.dtype))
            pieces.append(masked)
            if at + columns < LANES:
                pieces.append(jnp.zeros((LANES - at - columns, masked.shape[1]), masked.dtype))
            loads[slot * 2 + hemi].wait()
            total += lax.dot_general(
                leg_ref[slot, hemi * half : (hemi + 1) * half, :],
                jnp.concatenate(pieces, 0),
                NT,
                preferred_element_type=jnp.float32,
            )
    rows = jnp.dot(total.astype(jnp.bfloat16), perm_ref[...], preferred_element_type=jnp.float32)
    rows_ref[...] = rows * gain


def split_rows(dims, rows_ref, send_ref):
    quarter, half = dims["quarter"], dims["half"]
    for place in range(dims["groups"]):
        low = rows_ref[place * quarter : (place + 1) * quarter, :]
        top = half - place * quarter
        high = rows_ref[top - quarter : top, :]
        send_ref[place] = jnp.concatenate([low, high], 0).astype(jnp.bfloat16)


def whereabouts(dims, device, number):
    quarter, block = dims["quarter"], dims["block"]
    local = [number * block + u for u in range(block)]
    dist = [
        jnp.where(
            r < quarter, device * quarter + r, dims["half"] - (device + 2) * quarter + r
        )
        for r in local
    ]
    lengths = [20 + 4 * q for q in dist]
    return local, dist, lengths, [length.astype(jnp.float32) for length in lengths]


def tiles_of(longest):
    return (longest // 2 + POINTS) // POINTS


def most_tiles(dims):
    quarter, block, half = dims["quarter"], dims["block"], dims["half"]
    most = 0
    for device in range(dims["groups"]):
        total = 0
        for number in range(2 * quarter // block):
            r = number * block + block - 1
            q = device * quarter + r if r < quarter else half - (device + 2) * quarter + r
            total += tiles_of(20 + 4 * q)
        most = max(most, total)
    return most


def back_home(dims, part, slot, u):
    width = 2 * dims["waves"]
    if width >= LANES:
        return u * width + part * dims["waves"] + slot * dims["groups"]
    share = LANES // width
    inner = (part * dims["slots"] + slot) * share + u % share
    return u // share * LANES + inner * dims["groups"]


def lane_middle(value):
    return jnp.broadcast_to(value[:, LANES // 2 : LANES // 2 + 1], value.shape)


def prepare_stage(dims, device, degrees, quad_ref, cor_ref, partner, cor, scale):
    groups, half, quarter = dims["groups"], dims["half"], dims["quarter"]
    layers, block = dims["layers"], dims["block"]
    total_lat, count = 2 * half, 2 * quarter
    row = lax.broadcasted_iota(jnp.int32, (count, LANES), 0)
    dist = row + jnp.where(row < quarter, device * quarter, half - (device + 2) * quarter)
    length = (20 + 4 * dist).astype(jnp.float32)
    inverse = 1.0 / length
    lane = lax.broadcasted_iota(jnp.int32, (count, LANES), 1)
    cosine, sine = turn_trig(((degrees - 1) * lane).astype(jnp.float32), length, inverse)
    mid_cos, mid_sin = lane_middle(cosine), lane_middle(sine)
    partner[0], partner[1] = cosine, sine
    partner[2] = mid_cos * mid_cos - mid_sin * mid_sin
    partner[3] = 2.0 * mid_cos * mid_sin
    partner[4] = inverse
    north_row = lax.broadcasted_iota(jnp.int32, (2 * layers, LANES), 0) < layers
    wave_row = lax.broadcasted_iota(jnp.int32, (2 * layers, POINTS), 0) < layers
    width = 2 * dims["waves"]
    column = lax.broadcasted_iota(jnp.int32, (2 * layers, POINTS), 1)
    if width >= LANES:
        owner = column // width
    else:
        share = LANES // width
        owner = column // LANES * share + column // groups % share

    def group(number, carry):
        _, dist, _, floats = whereabouts(dims, device, number)
        scaled = jnp.zeros((2 * layers, POINTS), jnp.float32)
        for u, length in enumerate(floats):
            cor[number, u * 2 * layers : (u + 1) * 2 * layers, :] = jnp.where(
                north_row, cor_ref[dist[u]], cor_ref[total_lat - 1 - dist[u]]
            )
            here = jnp.where(wave_row, quad_ref[dist[u]], quad_ref[total_lat - 1 - dist[u]])
            scaled = jnp.where(owner == u, here / length, scaled)
        scale[number] = scaled
        return carry

    lax.fori_loop(0, count // block, group, 0)


def base_stage(dims, device, waves, partner, state, hop):
    groups, block = dims["groups"], dims["block"]
    lane = lax.broadcasted_iota(jnp.int32, (groups, LANES), 1).astype(jnp.float32)
    number = 2 * dims["quarter"] // block
    pace = 2 if number % 2 == 0 else 1

    def group(step, carry):
        for n in [step * pace + k for k in range(pace)]:
            floats = whereabouts(dims, device, n)[3]
            for u, length in enumerate(floats):
                full_cos, full_sin, jump_cos, jump_sin, inverse = [
                    jnp.broadcast_to(partner[k, pl.ds(n * block + u, 1), :], (groups, LANES))
                    for k in range(5)
                ]
                cosine, sine = turn_trig(waves[0] * lane, length, inverse)
                mid_cos, mid_sin = lane_middle(cosine), lane_middle(sine)
                turn_cos = mid_cos * mid_cos - mid_sin * mid_sin
                turn_sin = 2.0 * mid_cos * mid_sin
                keep = [jnp.where(2.0 * wave < length, 1.0, 0.0) for wave in waves]
                rows = slice(u * groups, (u + 1) * groups)
                state[n, 0, rows, :] = cosine * keep[0]
                state[n, 1, rows, :] = sine * keep[0]
                hop[n, 0, rows, :] = turn_cos
                hop[n, 1, rows, :] = turn_sin
                rows = slice((block + u) * groups, (block + u + 1) * groups)
                state[n, 0, rows, :] = (full_cos * cosine + full_sin * sine) * keep[1]
                state[n, 1, rows, :] = (full_sin * cosine - full_cos * sine) * keep[1]
                hop[n, 0, rows, :] = jump_cos * turn_cos + jump_sin * turn_sin
                hop[n, 1, rows, :] = jump_sin * turn_cos - jump_cos * turn_sin
        return carry

    lax.fori_loop(0, number // pace, group, 0)


def tile_list(dims, device):
    sizes = [
        tiles_of(whereabouts(dims, device, n)[2][-1])
        for n in range(2 * dims["quarter"] // dims["block"])
    ]
    ends = []
    for size in sizes:
        ends.append(size + (ends[-1] if ends else 0))
    return sizes, ends


def tile_at(tiles, item):
    number, start = 0, 0
    for size, end in zip(*tiles):
        number = number + jnp.where(item >= end, 1, 0)
        start = start + jnp.where(item >= end, size, 0)
    return number, item - start


def fill_tile(dims, device, tiles, item, place, state, hop, tab, back_tab):
    slots, groups, block = dims["slots"], dims["groups"], dims["block"]
    pair = min(2, block)
    wide = slots * block * groups
    sides = POINTS // LANES
    number, index = tile_at(tiles, item)
    length = whereabouts(dims, device, number)[3][0]
    lane = lax.broadcasted_iota(jnp.int32, (groups, LANES), 1).astype(jnp.float32)
    weight = []
    for side in range(sides):
        point = lane + (index * POINTS + side * LANES).astype(jnp.float32)
        start = jnp.minimum(point + 0.5, 1.0)
        reach = (0.5 * length + 0.5) - point
        each = [jnp.maximum(jnp.minimum(reach + 2.0 * u, start), 0.0) for u in range(block)]
        weight.append(
            [
                jnp.concatenate(each[u : u + pair], 0).astype(jnp.bfloat16)
                for u in range(0, block, pair)
            ]
        )
    for u in range(0, block, pair):
        for slot in range(slots):
            at = (slot * block + u) * groups
            rows = slice(at, at + pair * groups)
            cosine, sine = state[number, 0, rows, :], state[number, 1, rows, :]
            turn_cos, turn_sin = hop[number, 0, rows, :], hop[number, 1, rows, :]
            for side in range(sides):
                for part, value in enumerate((cosine, sine)):
                    packed = value.astype(jnp.bfloat16)
                    put = part * wide + at
                    tab[place, side, put : put + pair * groups, :] = packed
                    put = back_home(dims, part, slot, u)
                    back_tab[place, side, put : put + pair * groups, :] = (
                        packed * weight[side][u // pair]
                    )
                cosine, sine = (
                    cosine * turn_cos - sine * turn_sin,
                    sine * turn_cos + cosine * turn_sin,
                )
            state[number, 0, rows, :] = cosine
            state[number, 1, rows, :] = sine


def fill_stage(dims, device, tiles, state, hop, tab, back_tab):
    def body(step, carry):
        for k in range(FILLS):
            item = step * FILLS + k
            fill_tile(dims, device, tiles, item, item, state, hop, tab, back_tab)
        return carry

    lax.fori_loop(0, (tiles[1][-1] + FILLS - 1) // FILLS, body, 0)


def coefficient_stage(dims, get_ref, base, total):
    slots, groups, layers = dims["slots"], dims["groups"], dims["layers"]
    fields, block, count = dims["fields"], dims["block"], 2 * dims["quarter"]
    width = fields * 2 * layers
    number = count // block
    lane = lax.broadcasted_iota(jnp.int32, (groups, LANES), 1)
    south_lane = lane // layers % 2 == 1
    owner = lax.broadcasted_iota(jnp.int32, (width, LANES), 1)
    first_slot = owner < block * groups
    owner = owner // groups % block
    eye = (
        lax.broadcasted_iota(jnp.int32, (LANES, LANES), 0)
        == lax.broadcasted_iota(jnp.int32, (LANES, LANES), 1)
    ).astype(jnp.bfloat16)
    for start in range(0, number, 2):
        pieces = []
        for n in range(start, min(start + 2, number)):
            both = []
            for u in range(block):
                at = n * block + u
                north = get_ref[pl.ds(at, groups, stride=count), :]
                south = get_ref[pl.ds(count - 1 - at, groups, stride=count), :]
                both.append(jnp.where(south_lane, south, north))
            pieces += both * (LANES // (block * groups))
        turned = lax.dot_general(
            eye,
            jnp.concatenate(pieces, 0).astype(jnp.bfloat16),
            NT,
            preferred_element_type=jnp.float32,
        )
        for n in range(start, min(start + 2, number)):
            here = turned[:, (n - start) * LANES : (n - start + 1) * LANES]
            for part in range(2):
                value = [
                    here[(slot * 2 + part) * width : (slot * 2 + part + 1) * width]
                    for slot in range(slots)
                ]
                value = jnp.where(first_slot, value[0], value[1])
                for u in range(block):
                    mine = jnp.where(owner == u, value, 0.0)
                    near = (-mine if part else mine).astype(jnp.bfloat16)
                    base[n, part, u * 2 * width : (u * 2 + 1) * width, :] = near
                    far = mine.astype(jnp.bfloat16)
                    base[n, part, (u * 2 + 1) * width : (u * 2 + 2) * width, :] = far
    total[...] = jnp.zeros_like(total)


def side_by_side(ref, index):
    return jnp.concatenate([ref[index, side] for side in range(ref.shape[1])], 1)


def item_stage(dims, device, tiles, state, hop, base, tab, back_tab, cor, total):
    groups, layers, block = dims["groups"], dims["layers"], dims["block"]
    fields = dims["fields"]
    width = fields * 2 * layers
    rows = 2 * width
    span = 2 * dims["waves"]
    share = max(1, LANES // span)
    reach = max(LANES, span)
    across = lax.broadcasted_iota(jnp.int32, (width, reach), 1)
    sign = jnp.where(across // (reach // 2) == 0, 1.0, -1.0)

    def one(item, place):
        n = tile_at(tiles, item)[0]
        grid = jnp.dot(
            side_by_side(base, n), side_by_side(tab, place), preferred_element_type=jnp.float32
        )
        made = []
        for u in range(block):
            extra = cor[n, u * 2 * layers : (u + 1) * 2 * layers, :]
            extra = jnp.concatenate([extra] * (POINTS // LANES), 1)
            for side in range(2):
                at = (u * 2 + side) * width
                part = [
                    grid[at + f * 2 * layers : at + (f + 1) * 2 * layers] for f in range(fields)
                ]
                absolute = part[2] + extra
                made += [
                    absolute * part[0],
                    absolute * part[1],
                    0.5 * (part[0] * part[0] + part[1] * part[1]),
                    part[0] * part[3],
                ]
        products = jnp.concatenate(made, 0).astype(jnp.bfloat16)
        back = lax.dot_general(
            products, side_by_side(back_tab, place), NT, preferred_element_type=jnp.float32
        )
        for start in range(0, block, share):
            column = start * span // LANES * LANES
            joined = jnp.zeros((width, reach), jnp.float32)
            for u in range(start, min(start + share, block)):
                near = back[u * rows : u * rows + width, column : column + reach]
                far = back[u * rows + width : (u + 1) * rows, column : column + reach]
                value = near * sign + far
                keep = across // groups % share == u - start
                joined = value if share == 1 else jnp.where(keep, value, joined)
            total[n, :, column : column + reach] += joined

    def body(step, carry):
        for k in range(UNROLL):
            item = step * UNROLL + k
            one(item, item)
        return carry

    lax.fori_loop(0, (tiles[1][-1] + UNROLL - 1) // UNROLL, body, 0)


def return_stage(dims, total, scale, put_refs):
    slots, groups, layers = dims["slots"], dims["groups"], dims["layers"]
    fields, block, count = dims["fields"], dims["block"], 2 * dims["quarter"]
    width, span = fields * 2 * layers, 2 * dims["waves"]
    number = count // block
    share = max(1, LANES // span)
    lane = lax.broadcasted_iota(jnp.int32, (block * groups, POINTS), 1)
    row = lax.broadcasted_iota(jnp.int32, (block * groups, POINTS), 0)
    if span >= LANES:
        owner, kind = lane // span, lane % span // groups
    else:
        owner = lane // LANES * share + lane // groups % share
        kind = lane % LANES // (groups * share)
    pick = (owner * groups + lane % groups == row).astype(jnp.float32).astype(jnp.bfloat16)
    keep = []
    for slot in range(slots):
        for part in range(2):
            at = (kind[:1] == part * slots + slot).astype(jnp.float32)
            keep.append(jnp.broadcast_to(at, (width, POINTS)).astype(jnp.bfloat16))
    for start in range(0, number, 2):
        pieces = []
        for n in range(start, min(start + 2, number)):
            value = total[n] * jnp.concatenate([scale[n]] * fields, 0)
            value = value.astype(jnp.bfloat16)
            pieces += [value * here for here in keep]
        turned = lax.dot_general(
            pick, jnp.concatenate(pieces, 0), NT, preferred_element_type=jnp.float32
        )
        for n in range(start, min(start + 2, number)):
            for u in range(block):
                at = n * block + u
                value = turned[
                    u * groups : (u + 1) * groups, (n - start) * LANES : (n - start + 1) * LANES
                ]
                put_refs[0][pl.ds(at, groups, stride=count), :] = value
                put_refs[1][pl.ds(count - 1 - at, groups, stride=count), :] = value


def grid_scratch(dims):
    slots, groups, block = dims["slots"], dims["groups"], dims["block"]
    layers, fields = dims["layers"], dims["fields"]
    number = 2 * dims["quarter"] // block
    wide = slots * block * groups
    width = fields * 2 * layers
    items = -(-most_tiles(dims) // UNROLL) * UNROLL
    return [
        pltpu.VMEM((5, number * block, LANES), jnp.float32),
        pltpu.VMEM((number + 1, 2, wide, LANES), jnp.float32),
        pltpu.VMEM((number + 1, 2, wide, LANES), jnp.float32),
        pltpu.VMEM((items, POINTS // LANES, 2 * wide, LANES), jnp.bfloat16),
        pltpu.VMEM((items, POINTS // LANES, 2 * wide, LANES), jnp.bfloat16),
        pltpu.VMEM((number + 1, block * 2 * layers, LANES), jnp.float32),
        pltpu.VMEM((number, 2 * layers, POINTS), jnp.float32),
        pltpu.VMEM((number + 1, 2, block * 2 * width, wide), jnp.bfloat16),
        pltpu.VMEM((number + 1, width, 2 * wide), jnp.float32),
    ]


def final_stage(dims, get, leg_ref, perm_ref):
    slots, columns, half = dims["slots"], dims["columns"], dims["half"]
    turned = lax.dot_general(
        perm_ref[...], get, NT, preferred_element_type=jnp.float32
    ).astype(jnp.bfloat16)
    results = []
    for slot in range(slots):
        total = 0.0
        for hemi in range(2):
            at = (slot * 2 + hemi) * columns
            total += jnp.dot(
                turned[at : at + columns],
                leg_ref[slot, hemi * half : (hemi + 1) * half, :],
                preferred_element_type=jnp.float32,
            )
        results.append(total)
    return results


def joined_rows(dims, back_ref):
    quarter, groups = dims["quarter"], dims["groups"]
    low = [back_ref[place][:quarter] for place in range(groups)]
    high = [back_ref[place][quarter:] for place in reversed(range(groups))]
    return low + high


def to_peer(axis, shift):
    place = lax.axis_index(axis)
    count = lax.axis_size(axis)
    return {axis: lax.rem(place + shift, count)}


def exchange(axis, source_of, target_of, sems):
    place = lax.axis_index(axis)
    count = lax.axis_size(axis)
    copies = []
    for shift in range(1, count):
        peer = lax.rem(place + shift, count)
        copies.append(
            pltpu.make_async_remote_copy(
                src_ref=source_of(peer),
                dst_ref=target_of(place),
                send_sem=sems[0].at[shift],
                recv_sem=sems[1].at[shift],
                device_id=to_peer(axis, shift),
                device_id_type=pl.DeviceIdType.MESH,
            )
        )
    return copies


def whole_kernel(
    dims, spec_hbm, leg_hbm, perm_hbm, share_hbm, quad_hbm, cor_hbm, wave_hbm, out_ref,
    spec_ref, perm_ref, share_ref, quad_ref, cor_ref, wave_ref, in_sem,
    leg, rows, send, recv, back_send, back, wave_send, wave_recv, sum_send, sum_recv, geo,
    get, north, south, load_sem, sem_a, sem_b, sem_c, sem_d, sem_e, sem_f, sem_g, sem_h, *scratch,
):
    slots, groups, half = dims["slots"], dims["groups"], dims["half"]
    fields, layers, count = dims["fields"], dims["layers"], 2 * dims["quarter"]
    degrees = spec_hbm.shape[2]
    me = lax.axis_index("wave")
    floor = lax.axis_index("lev")
    floors = lax.axis_size("lev")
    pairs = (
        (spec_hbm, spec_ref), (wave_hbm, wave_ref), (share_hbm, share_ref),
        (perm_hbm, perm_ref), (quad_hbm, quad_ref), (cor_hbm, cor_ref),
    )
    brought = [
        pltpu.make_async_copy(source, target, in_sem.at[k])
        for k, (source, target) in enumerate(pairs)
    ]
    for copy in brought:
        copy.start()
    loads = []
    for slot in range(slots):
        for hemi in range(2):
            piece = pl.ds(hemi * half, half)
            copy = pltpu.make_async_copy(
                leg_hbm.at[slot, piece], leg.at[slot, piece], load_sem.at[slot * 2 + hemi]
            )
            copy.start()
            loads.append(copy)
    barrier = pltpu.get_barrier_semaphore()
    for shift in range(1, groups):
        pl.semaphore_signal(
            barrier, inc=1, device_id=to_peer("wave", shift), device_id_type=pl.DeviceIdType.MESH
        )

    @pl.when(floor < floors - 1)
    def _():
        pl.semaphore_signal(
            barrier, inc=1, device_id={"lev": floor + 1}, device_id_type=pl.DeviceIdType.MESH
        )

    for copy in brought:
        copy.wait()
    degree = lax.broadcasted_iota(jnp.int32, (1, degrees), 1)
    live = [
        jnp.where(degree < degrees - wave_ref[slot], 1.0, 0.0).astype(jnp.float32)
        for slot in range(slots)
    ]
    row = lax.broadcasted_iota(jnp.int32, (8, LANES), 0)
    own = jnp.zeros((8, LANES), jnp.float32)
    for slot in range(slots):
        own = jnp.where(row == slot, wave_ref[slot].astype(jnp.float32), own)
    wave_send[...] = own
    geo[...] = jnp.zeros_like(geo)
    for slot in range(slots):
        full = spec_ref[slot].astype(jnp.float32) * live[slot]
        for part in range(2):
            first = part * fields * layers
            total = jnp.zeros((1, degrees), jnp.float32)
            for layer in reversed(range(layers)):
                at = first + 3 * layers + layer
                total = total + full[at : at + 1] * share_ref[layer]
                at = first + 2 * layers + layer
                geo[slot, at : at + 1, :] = total
            at = slot * 2 + part
            sum_send[at : at + 1, :] = total
    place = lax.broadcasted_iota(jnp.int32, (1, LANES), 1) // (LANES // slots)
    gain = jnp.ones((1, LANES), jnp.float32)
    for slot in range(slots):
        twice = jnp.where(wave_ref[slot] == 0, 1.0, 2.0)
        gain = jnp.where(place == slot, twice, gain)
    fourier_stage(dims, spec_ref, leg, loads, live, gain, perm_ref, rows)
    split_rows(dims, rows, send)
    pl.semaphore_wait(barrier, groups - 1 + jnp.where(floor > 0, 1, 0))

    def wave_place(device):
        return wave_recv.at[pl.ds(pl.multiple_of(device * 8, 8), 8)]

    tell = exchange("wave", lambda _: wave_send, wave_place, (sem_a, sem_b))
    lift = [
        pltpu.make_async_remote_copy(
            src_ref=sum_recv.at[step - 1] if step else sum_send,
            dst_ref=sum_recv.at[step],
            send_sem=sem_c.at[step],
            recv_sem=sem_d.at[step],
            device_id={"lev": lax.rem(floor + floors - 1, floors)},
            device_id_type=pl.DeviceIdType.MESH,
        )
        for step in range(floors - 1)
    ]

    def raise_sums(step):
        if step:

            @pl.when(floor + step < floors)
            def _():
                lift[step - 1].wait_recv()

        if step < floors - 1:

            @pl.when((floor > 0) & (floor + step < floors))
            def _():
                lift[step].start()

    for copy in tell:
        copy.start()
    wave_recv[pl.ds(pl.multiple_of(me * 8, 8), 8), :] = own
    there = exchange("wave", lambda p: send.at[p], lambda p: recv.at[p], (sem_e, sem_f))
    for copy in there:
        copy.start()
    raise_sums(0)
    recv[me] = send[me]
    partner, state, hop, tab, back_tab, cor, scale, base, total = scratch
    prepare_stage(dims, me, degrees, quad_ref, cor_ref, partner, cor, scale)
    tiles = tile_list(dims, me)
    for copy in tell:
        copy.wait()
    waves = [wave_recv[pl.ds(slot, groups, stride=8), :] for slot in range(slots)]
    base_stage(dims, me, waves, partner, state, hop)
    raise_sums(1)
    fill_stage(dims, me, tiles, state, hop, tab, back_tab)
    for copy in there:
        copy.wait()
    for source in range(groups):
        get[source * count : (source + 1) * count, :] = recv[source].astype(jnp.float32)
    coefficient_stage(dims, get, base, total)
    if floors > 2:
        raise_sums(2)
    item_stage(dims, me, tiles, state, hop, base, tab, back_tab, cor, total)
    return_stage(dims, total, scale, (north, south))
    hemi = lax.broadcasted_iota(jnp.int32, (count, LANES), 1) // layers % 2
    for source in range(groups):
        piece = slice(source * count, (source + 1) * count)
        back_send[source] = jnp.where(hemi == 1, south[piece], north[piece]).astype(jnp.bfloat16)
    home = exchange("wave", lambda p: back_send.at[p], lambda p: back.at[p], (sem_g, sem_h))
    for copy in home:
        copy.start()
    back[me] = back_send[me]
    for step in range(3, floors):
        raise_sums(step)
    for step in range(floors - 1):

        @pl.when((floor > 0) & (floor + step < floors))
        def _():
            lift[step].wait_send()

    for slot in range(slots):
        for part in range(2):
            at = slot * 2 + part
            deeper = jnp.zeros((1, degrees), jnp.float32)
            for step in range(floors - 1):
                value = sum_recv[step, at : at + 1, :]
                deeper = deeper + jnp.where(floor + step + 1 < floors, value, 0.0)
            first = (part * fields + 2) * layers
            geo[slot, first : first + layers, :] += deeper
    for copy in home:
        copy.wait()
    pieces = [piece.astype(jnp.float32) for piece in joined_rows(dims, back)]
    joined = jnp.concatenate(pieces, 0).astype(jnp.bfloat16)
    for slot, value in enumerate(final_stage(dims, joined, leg, perm_ref)):
        out_ref[slot] = ((value + geo[slot]) * live[slot]).astype(jnp.bfloat16)


def body(spec, legendre, layer_depth_share, quad_weight, wave_of_slot):
    slots, columns, degrees = spec.shape
    total_lat = legendre.shape[1]
    groups = lax.axis_size("wave")
    layers = layer_depth_share.shape[0]
    quarter = total_lat // groups // 4
    depth = 2 * slots * groups
    block = max(b for b in range(1, quarter + 1) if quarter % b == 0 and b * depth <= max(256, depth))
    dims = dict(
        slots=slots, columns=columns, half=total_lat // 2, groups=groups, layers=layers,
        fields=columns // (2 * layers), quarter=quarter, block=block, waves=slots * groups,
    )
    fields = dims["fields"]
    maps = lane_maps(slots, fields, layers)
    perm = np.zeros((LANES, LANES), np.float32)
    perm[maps, np.arange(LANES)] = 1.0
    perm = jnp.asarray(perm, jnp.bfloat16)
    lat = np.arange(total_lat)
    coriolis = jnp.asarray(2.0 * np.cos(np.pi * (lat + 0.5) / total_lat), jnp.float32)
    floors = lax.axis_size("lev")
    half, count = total_lat // 2, 2 * quarter
    vmem = pl.BlockSpec(memory_space=pltpu.VMEM)
    rows = pltpu.VMEM((groups, count, LANES), jnp.bfloat16)
    flat = pltpu.VMEM((groups * count, LANES), jnp.float32)
    sums = 2 * slots
    operands = (spec, legendre, perm, layer_depth_share, quad_weight, coriolis, wave_of_slot)
    operands = [pltpu.with_memory_space_constraint(x, pltpu.HBM) for x in operands]
    return pl.pallas_call(
        functools.partial(whole_kernel, dims),
        out_shape=jax.ShapeDtypeStruct(spec.shape, jnp.bfloat16),
        in_specs=[pl.BlockSpec(memory_space=pltpu.HBM)] * len(operands),
        out_specs=vmem,
        scratch_shapes=[
            pltpu.VMEM(spec.shape, jnp.bfloat16),
            pltpu.VMEM((LANES, LANES), jnp.bfloat16),
            pltpu.SMEM(layer_depth_share.shape, jnp.float32),
            pltpu.SMEM(quad_weight.shape, jnp.float32),
            pltpu.SMEM(quad_weight.shape, jnp.float32),
            pltpu.SMEM(wave_of_slot.shape, jnp.int32),
            pltpu.SemaphoreType.DMA((6,)),
            pltpu.VMEM(legendre.shape, jnp.bfloat16),
            pltpu.VMEM((half, LANES), jnp.float32),
            rows, rows, rows, rows,
            pltpu.VMEM((8, LANES), jnp.float32),
            pltpu.VMEM((groups * 8, LANES), jnp.float32),
            pltpu.VMEM((sums, degrees), jnp.float32),
            pltpu.VMEM((floors, sums, degrees), jnp.float32),
            pltpu.VMEM(spec.shape, jnp.float32),
            flat, flat, flat,
            pltpu.SemaphoreType.DMA((2 * slots,)),
            pltpu.SemaphoreType.DMA((groups,)),
            pltpu.SemaphoreType.DMA((groups,)),
            pltpu.SemaphoreType.DMA((floors,)),
            pltpu.SemaphoreType.DMA((floors,)),
            pltpu.SemaphoreType.DMA((groups,)),
            pltpu.SemaphoreType.DMA((groups,)),
            pltpu.SemaphoreType.DMA((groups,)),
            pltpu.SemaphoreType.DMA((groups,)),
        ]
        + grid_scratch(dims),
        compiler_params=pltpu.CompilerParams(collective_id=0, has_side_effects=True, vmem_limit_bytes=VMEM_BYTES),
    )(*operands)


def solution(mesh):
    in_specs = (P("wave", "lev", None), P("wave", None, None), P("lev"), P(), P("wave"))
    out_specs = P("wave", "lev", None)
    return jax.shard_map(body, mesh=mesh, in_specs=in_specs, out_specs=out_specs, check_vma=False)
```

```python
import functools
import math

import jax
import jax.numpy as jnp
import numpy as np
from jax import lax
from jax.experimental import pallas as pl
from jax.experimental.pallas import tpu as pltpu
from jax.sharding import PartitionSpec as P

LANES = 128
POINTS = 2 * LANES
UNROLL = 32
FILLS = 4
VMEM_BYTES = 48 * 2**20
NT = (((1,), (1,)), ((), ()))


def taylor(first, count):
    return [(-1.0) ** k / math.factorial(2 * k + first) for k in range(count)]


def horner(square, terms):
    total = jnp.full_like(square, terms[-1])
    for term in reversed(terms[:-1]):
        total = total * square + term
    return total


def turn_trig(steps, length, inverse):
    whole = jnp.floor(steps * inverse + 0.5)
    angle = (steps - whole * length) * (inverse * math.pi)
    square = angle * angle
    sine = angle * horner(square, taylor(1, 6))
    twice = sine + sine
    return 1.0 - twice * sine, twice * horner(square, taylor(0, 7))


def lane_maps(slots, fields, layers):
    order = np.arange(slots * 2 * 2 * fields * layers)
    natural = order.reshape(slots, 2, 2, fields, layers)
    return natural.transpose(0, 2, 3, 1, 4).reshape(-1)


def spread_rows(dims, hemi, masked):
    layers = dims["layers"]
    row = lax.broadcasted_iota(jnp.int32, (2 * layers, masked.shape[1]), 0)
    keep = row // layers == hemi
    pieces = []
    for at in range(0, masked.shape[0], 2 * layers):
        here = masked[at : at + 2 * layers]
        turned = pltpu.roll(here, layers, 0)
        pieces += [turned, here] if hemi else [here, turned]
    return jnp.concatenate([jnp.where(keep, piece, 0.0) for piece in pieces], 0)


def fourier_stage(dims, full, leg_ref, loads, gain, rows_ref):
    slots, half = dims["slots"], dims["half"]
    total = 0.0
    for hemi in range(2):
        weights = []
        for slot in range(slots):
            mine = spread_rows(dims, hemi, full[slot]).astype(jnp.bfloat16)
            blank = jnp.zeros_like(mine)
            weights.append(
                jnp.concatenate([mine if k == slot else blank for k in range(slots)], 1)
            )
        weights = jnp.concatenate(weights, 0)
        for slot in range(slots):
            loads[slot * 2 + hemi].wait()
        table = [leg_ref[slot, hemi * half : (hemi + 1) * half, :] for slot in range(slots)]
        total += lax.dot_general(
            jnp.concatenate(table, 1), weights, NT, preferred_element_type=jnp.float32
        )
    rows_ref[...] = total * gain


def split_rows(dims, rows_ref, send_ref):
    quarter, half = dims["quarter"], dims["half"]
    for place in range(dims["groups"]):
        low = rows_ref[place * quarter : (place + 1) * quarter, :]
        top = half - place * quarter
        high = rows_ref[top - quarter : top, :]
        send_ref[place] = jnp.concatenate([low, high], 0).astype(jnp.bfloat16)


def whereabouts(dims, device, number):
    quarter, block = dims["quarter"], dims["block"]
    local = [number * block + u for u in range(block)]
    dist = [
        jnp.where(
            r < quarter, device * quarter + r, dims["half"] - (device + 2) * quarter + r
        )
        for r in local
    ]
    lengths = [20 + 4 * q for q in dist]
    return local, dist, lengths, [length.astype(jnp.float32) for length in lengths]


def tiles_of(longest):
    return (longest // 2 + POINTS) // POINTS


def most_tiles(dims):
    quarter, block, half = dims["quarter"], dims["block"], dims["half"]
    most = 0
    for device in range(dims["groups"]):
        total = 0
        for number in range(2 * quarter // block):
            r = number * block + block - 1
            q = device * quarter + r if r < quarter else half - (device + 2) * quarter + r
            total += tiles_of(20 + 4 * q)
        most = max(most, total)
    return most


def back_home(dims, part, slot, u):
    width = 2 * dims["waves"]
    if width >= LANES:
        return u * width + part * dims["waves"] + slot * dims["groups"]
    share = LANES // width
    inner = (part * dims["slots"] + slot) * share + u % share
    return u // share * LANES + inner * dims["groups"]


def lane_middle(value):
    return jnp.broadcast_to(value[:, LANES // 2 : LANES // 2 + 1], value.shape)


def prepare_stage(dims, device, degrees, quad_ref, cor_ref, partner, cor, scale):
    groups, half, quarter = dims["groups"], dims["half"], dims["quarter"]
    layers, block = dims["layers"], dims["block"]
    total_lat, count = 2 * half, 2 * quarter
    row = lax.broadcasted_iota(jnp.int32, (count, LANES), 0)
    dist = row + jnp.where(row < quarter, device * quarter, half - (device + 2) * quarter)
    length = (20 + 4 * dist).astype(jnp.float32)
    inverse = 1.0 / length
    lane = lax.broadcasted_iota(jnp.int32, (count, LANES), 1)
    cosine, sine = turn_trig(((degrees - 1) * lane).astype(jnp.float32), length, inverse)
    mid_cos, mid_sin = lane_middle(cosine), lane_middle(sine)
    partner[0], partner[1] = cosine, sine
    partner[2] = mid_cos * mid_cos - mid_sin * mid_sin
    partner[3] = 2.0 * mid_cos * mid_sin
    partner[4] = inverse
    north_row = lax.broadcasted_iota(jnp.int32, (2 * layers, LANES), 0) < layers
    wave_row = lax.broadcasted_iota(jnp.int32, (2 * layers, POINTS), 0) < layers
    width = 2 * dims["waves"]
    column = lax.broadcasted_iota(jnp.int32, (2 * layers, POINTS), 1)
    if width >= LANES:
        owner = column // width
    else:
        share = LANES // width
        owner = column // LANES * share + column // groups % share

    def group(number, carry):
        _, dist, _, floats = whereabouts(dims, device, number)
        scaled = jnp.zeros((2 * layers, POINTS), jnp.float32)
        for u, length in enumerate(floats):
            cor[number, u * 2 * layers : (u + 1) * 2 * layers, :] = jnp.where(
                north_row, cor_ref[dist[u]], cor_ref[total_lat - 1 - dist[u]]
            )
            here = jnp.where(wave_row, quad_ref[dist[u]], quad_ref[total_lat - 1 - dist[u]])
            scaled = jnp.where(owner == u, here / length, scaled)
        scale[number] = scaled
        return carry

    lax.fori_loop(0, count // block, group, 0)


def base_stage(dims, device, waves, partner, state, hop):
    groups, block = dims["groups"], dims["block"]
    lane = lax.broadcasted_iota(jnp.int32, (groups, LANES), 1).astype(jnp.float32)
    number = 2 * dims["quarter"] // block
    pace = 2 if number % 2 == 0 else 1

    def group(step, carry):
        for n in [step * pace + k for k in range(pace)]:
            floats = whereabouts(dims, device, n)[3]
            for u, length in enumerate(floats):
                full_cos, full_sin, jump_cos, jump_sin, inverse = [
                    jnp.broadcast_to(partner[k, pl.ds(n * block + u, 1), :], (groups, LANES))
                    for k in range(5)
                ]
                cosine, sine = turn_trig(waves[0] * lane, length, inverse)
                mid_cos, mid_sin = lane_middle(cosine), lane_middle(sine)
                turn_cos = mid_cos * mid_cos - mid_sin * mid_sin
                turn_sin = 2.0 * mid_cos * mid_sin
                keep = [jnp.where(2.0 * wave < length, 1.0, 0.0) for wave in waves]
                rows = slice(u * groups, (u + 1) * groups)
                state[n, 0, rows, :] = cosine * keep[0]
                state[n, 1, rows, :] = sine * keep[0]
                hop[n, 0, rows, :] = turn_cos
                hop[n, 1, rows, :] = turn_sin
                rows = slice((block + u) * groups, (block + u + 1) * groups)
                state[n, 0, rows, :] = (full_cos * cosine + full_sin * sine) * keep[1]
                state[n, 1, rows, :] = (full_sin * cosine - full_cos * sine) * keep[1]
                hop[n, 0, rows, :] = jump_cos * turn_cos + jump_sin * turn_sin
                hop[n, 1, rows, :] = jump_sin * turn_cos - jump_cos * turn_sin
        return carry

    lax.fori_loop(0, number // pace, group, 0)


def tile_list(dims, device):
    sizes = [
        tiles_of(whereabouts(dims, device, n)[2][-1])
        for n in range(2 * dims["quarter"] // dims["block"])
    ]
    ends = []
    for size in sizes:
        ends.append(size + (ends[-1] if ends else 0))
    return sizes, ends


def tile_at(tiles, item):
    number, start = 0, 0
    for size, end in zip(*tiles):
        number = number + jnp.where(item >= end, 1, 0)
        start = start + jnp.where(item >= end, size, 0)
    return number, item - start


def fill_tile(dims, device, tiles, item, place, state, hop, tab, back_tab):
    slots, groups, block = dims["slots"], dims["groups"], dims["block"]
    pair = min(2, block)
    wide = slots * block * groups
    sides = POINTS // LANES
    number, index = tile_at(tiles, item)
    length = whereabouts(dims, device, number)[3][0]
    lane = lax.broadcasted_iota(jnp.int32, (groups, LANES), 1).astype(jnp.float32)
    weight = []
    for side in range(sides):
        point = lane + (index * POINTS + side * LANES).astype(jnp.float32)
        start = jnp.minimum(point + 0.5, 1.0)
        reach = (0.5 * length + 0.5) - point
        each = [jnp.maximum(jnp.minimum(reach + 2.0 * u, start), 0.0) for u in range(block)]
        weight.append(
            [
                jnp.concatenate(each[u : u + pair], 0)
                for u in range(0, block, pair)
            ]
        )
    for u in range(0, block, pair):
        for slot in range(slots):
            at = (slot * block + u) * groups
            rows = slice(at, at + pair * groups)
            cosine, sine = state[number, 0, rows, :], state[number, 1, rows, :]
            turn_cos, turn_sin = hop[number, 0, rows, :], hop[number, 1, rows, :]
            for side in range(sides):
                for part, value in enumerate((cosine, sine)):
                    put = part * wide + at
                    tab[place, side, put : put + pair * groups, :] = value.astype(jnp.bfloat16)
                    put = back_home(dims, part, slot, u)
                    back_tab[place, side, put : put + pair * groups, :] = (
                        value * weight[side][u // pair]
                    ).astype(jnp.bfloat16)
                cosine, sine = (
                    cosine * turn_cos - sine * turn_sin,
                    sine * turn_cos + cosine * turn_sin,
                )
            state[number, 0, rows, :] = cosine
            state[number, 1, rows, :] = sine


def fill_stage(dims, device, tiles, state, hop, tab, back_tab):
    def body(step, carry):
        for k in range(FILLS):
            item = step * FILLS + k
            fill_tile(dims, device, tiles, item, item, state, hop, tab, back_tab)
        return carry

    lax.fori_loop(0, (tiles[1][-1] + FILLS - 1) // FILLS, body, 0)


def coefficient_stage(dims, get_ref, base, total):
    slots, groups, layers = dims["slots"], dims["groups"], dims["layers"]
    fields, block, count = dims["fields"], dims["block"], 2 * dims["quarter"]
    width = fields * 2 * layers
    number = count // block
    lane = lax.broadcasted_iota(jnp.int32, (groups, LANES), 1)
    south_lane = lane // layers % 2 == 1
    first_slot = lax.broadcasted_iota(jnp.int32, (width, LANES), 1) < block * groups
    eye = (
        lax.broadcasted_iota(jnp.int32, (LANES, LANES), 0)
        == lax.broadcasted_iota(jnp.int32, (LANES, LANES), 1)
    ).astype(jnp.bfloat16)
    for start in range(0, number, 2):
        pieces = []
        for n in range(start, min(start + 2, number)):
            both = []
            for u in range(block):
                at = n * block + u
                north = get_ref[pl.ds(at, groups, stride=count), :]
                south = get_ref[pl.ds(count - 1 - at, groups, stride=count), :]
                both.append(jnp.where(south_lane, south, north))
            pieces += both * (LANES // (block * groups))
        turned = lax.dot_general(
            eye,
            jnp.concatenate(pieces, 0).astype(jnp.bfloat16),
            NT,
            preferred_element_type=jnp.float32,
        )
        for n in range(start, min(start + 2, number)):
            here = turned[:, (n - start) * LANES : (n - start + 1) * LANES]
            for part in range(2):
                value = [
                    here[(slot * 2 + part) * width : (slot * 2 + part + 1) * width]
                    for slot in range(slots)
                ]
                value = jnp.where(first_slot, value[0], value[1])
                base[n, part] = value.astype(jnp.bfloat16)
    total[...] = jnp.zeros_like(total)


def side_by_side(ref, index):
    return jnp.concatenate([ref[index, side] for side in range(ref.shape[1])], 1)


def item_stage(dims, device, tiles, state, hop, base, tab, back_tab, cor, total):
    groups, layers, block = dims["groups"], dims["layers"], dims["block"]
    fields = dims["fields"]
    width = fields * 2 * layers
    rows = 2 * width
    lane = lax.broadcasted_iota(jnp.int32, (width, LANES), 1)
    mine = [
        (lane // groups % block == u).astype(jnp.float32).astype(jnp.bfloat16)
        for u in range(block)
    ]
    span = 2 * dims["waves"]
    share = max(1, LANES // span)
    reach = max(LANES, span)
    across = lax.broadcasted_iota(jnp.int32, (width, reach), 1)
    sign = jnp.where(across // (reach // 2) == 0, 1.0, -1.0)

    def one(item, place):
        n = tile_at(tiles, item)[0]
        pieces = []
        for u in range(block):
            left, right = base[n, 0] * mine[u], base[n, 1] * mine[u]
            pieces.append(jnp.concatenate([left, -right], 1))
            pieces.append(jnp.concatenate([left, right], 1))
        grid = jnp.dot(
            jnp.concatenate(pieces, 0),
            side_by_side(tab, place),
            preferred_element_type=jnp.float32,
        )
        made = []
        for u in range(block):
            extra = cor[n, u * 2 * layers : (u + 1) * 2 * layers, :]
            extra = jnp.concatenate([extra] * (POINTS // LANES), 1)
            for side in range(2):
                at = (u * 2 + side) * width
                part = [
                    grid[at + f * 2 * layers : at + (f + 1) * 2 * layers] for f in range(fields)
                ]
                absolute = part[2] + extra
                made += [
                    absolute * part[0],
                    absolute * part[1],
                    0.5 * (part[0] * part[0] + part[1] * part[1]),
                    part[0] * part[3],
                ]
        products = jnp.concatenate(made, 0).astype(jnp.bfloat16)
        back = lax.dot_general(
            products, side_by_side(back_tab, place), NT, preferred_element_type=jnp.float32
        )
        for start in range(0, block, share):
            column = start * span // LANES * LANES
            joined = jnp.zeros((width, reach), jnp.float32)
            for u in range(start, min(start + share, block)):
                near = back[u * rows : u * rows + width, column : column + reach]
                far = back[u * rows + width : (u + 1) * rows, column : column + reach]
                value = near * sign + far
                keep = across // groups % share == u - start
                joined = value if share == 1 else jnp.where(keep, value, joined)
            total[n, :, column : column + reach] += joined

    def body(step, carry):
        for k in range(UNROLL):
            item = step * UNROLL + k
            one(item, item)
        return carry

    lax.fori_loop(0, (tiles[1][-1] + UNROLL - 1) // UNROLL, body, 0)


def return_stage(dims, total, scale, put_refs):
    slots, groups, layers = dims["slots"], dims["groups"], dims["layers"]
    fields, block, count = dims["fields"], dims["block"], 2 * dims["quarter"]
    width, span = fields * 2 * layers, 2 * dims["waves"]
    number = count // block
    share = max(1, LANES // span)
    lane = lax.broadcasted_iota(jnp.int32, (block * groups, POINTS), 1)
    row = lax.broadcasted_iota(jnp.int32, (block * groups, POINTS), 0)
    if span >= LANES:
        owner, kind = lane // span, lane % span // groups
    else:
        owner = lane // LANES * share + lane // groups % share
        kind = lane % LANES // (groups * share)
    pick = (owner * groups + lane % groups == row).astype(jnp.float32).astype(jnp.bfloat16)
    keep = []
    for slot in range(slots):
        for part in range(2):
            at = (kind[:1] == part * slots + slot).astype(jnp.float32)
            keep.append(jnp.broadcast_to(at, (width, POINTS)).astype(jnp.bfloat16))
    for start in range(0, number, 2):
        pieces = []
        for n in range(start, min(start + 2, number)):
            value = total[n] * jnp.concatenate([scale[n]] * fields, 0)
            value = value.astype(jnp.bfloat16)
            pieces += [value * here for here in keep]
        turned = lax.dot_general(
            pick, jnp.concatenate(pieces, 0), NT, preferred_element_type=jnp.float32
        )
        for n in range(start, min(start + 2, number)):
            for u in range(block):
                at = n * block + u
                value = turned[
                    u * groups : (u + 1) * groups, (n - start) * LANES : (n - start + 1) * LANES
                ]
                put_refs[0][pl.ds(at, groups, stride=count), :] = value
                put_refs[1][pl.ds(count - 1 - at, groups, stride=count), :] = value


def grid_scratch(dims):
    slots, groups, block = dims["slots"], dims["groups"], dims["block"]
    layers, fields = dims["layers"], dims["fields"]
    number = 2 * dims["quarter"] // block
    wide = slots * block * groups
    width = fields * 2 * layers
    items = -(-most_tiles(dims) // UNROLL) * UNROLL
    return [
        pltpu.VMEM((5, number * block, LANES), jnp.float32),
        pltpu.VMEM((number + 1, 2, wide, LANES), jnp.float32),
        pltpu.VMEM((number + 1, 2, wide, LANES), jnp.float32),
        pltpu.VMEM((items, POINTS // LANES, 2 * wide, LANES), jnp.bfloat16),
        pltpu.VMEM((items, POINTS // LANES, 2 * wide, LANES), jnp.bfloat16),
        pltpu.VMEM((number + 1, block * 2 * layers, LANES), jnp.float32),
        pltpu.VMEM((number, 2 * layers, POINTS), jnp.float32),
        pltpu.VMEM((number + 1, 2, width, wide), jnp.bfloat16),
        pltpu.VMEM((number + 1, width, 2 * wide), jnp.float32),
    ]


def final_stage(dims, get, leg_ref, perm_ref):
    slots, columns = dims["slots"], dims["columns"]
    turned = lax.dot_general(
        perm_ref[...], get, NT, preferred_element_type=jnp.float32
    ).astype(jnp.bfloat16)
    results = []
    for slot in range(slots):
        rows = [
            turned[(slot * 2 + hemi) * columns : (slot * 2 + hemi + 1) * columns]
            for hemi in range(2)
        ]
        total = jnp.dot(
            jnp.concatenate(rows, 1), leg_ref[slot], preferred_element_type=jnp.float32
        )
        results.append(total)
    return results


def joined_rows(dims, back_ref):
    quarter, groups = dims["quarter"], dims["groups"]
    low = [back_ref[place][:quarter] for place in range(groups)]
    high = [back_ref[place][quarter:] for place in reversed(range(groups))]
    return low + high


def to_peer(axis, shift):
    place = lax.axis_index(axis)
    count = lax.axis_size(axis)
    return {axis: lax.rem(place + shift, count)}


def far_first(count):
    if count & (count - 1):
        return list(range(1, count))
    return sorted(range(1, count), key=lambda d: (-bin(d >> 1).count("1"), d))


def partner_of(place, count, step):
    if count & (count - 1):
        return lax.rem(place + step, count)
    peer, bit = place, 1
    while bit < count:
        if step & bit:
            peer = peer + bit * (1 - 2 * lax.rem(lax.div(place, bit), 2))
        bit *= 2
    return peer


def exchange(axis, source_of, target_of, sems):
    place = lax.axis_index(axis)
    count = lax.axis_size(axis)
    copies = []
    for step in far_first(count):
        peer = partner_of(place, count, step)
        copies.append(
            pltpu.make_async_remote_copy(
                src_ref=source_of(peer),
                dst_ref=target_of(place),
                send_sem=sems.at[0],
                recv_sem=sems.at[1],
                device_id={axis: peer},
                device_id_type=pl.DeviceIdType.MESH,
            )
        )
    return copies


def all_of(axis, source, target, sems):
    return pltpu.make_async_remote_copy(
        src_ref=source,
        dst_ref=target,
        send_sem=sems.at[0],
        recv_sem=sems.at[1],
        device_id=to_peer(axis, 1),
        device_id_type=pl.DeviceIdType.MESH,
    )


def whole_kernel(
    dims, spec_hbm, leg_hbm, perm_hbm, share_hbm, quad_hbm, cor_hbm, wave_hbm, out_ref,
    spec_ref, perm_ref, share_ref, quad_ref, cor_ref, wave_ref, in_sem,
    leg, rows, send, recv, back_send, back, wave_send, wave_recv, sum_send, sum_recv, geo,
    get, north, south, load_sem, tell_sem, sem_c, sem_d, there_sem, home_sem, *scratch,
):
    slots, groups, half = dims["slots"], dims["groups"], dims["half"]
    fields, layers, count = dims["fields"], dims["layers"], 2 * dims["quarter"]
    degrees = spec_hbm.shape[2]
    me = lax.axis_index("wave")
    floor = lax.axis_index("lev")
    floors = lax.axis_size("lev")
    barrier = pltpu.get_barrier_semaphore()
    for step in far_first(groups):
        pl.semaphore_signal(
            barrier,
            inc=1,
            device_id={"wave": partner_of(me, groups, step)},
            device_id_type=pl.DeviceIdType.MESH,
        )

    @pl.when(floor < floors - 1)
    def _():
        pl.semaphore_signal(
            barrier, inc=1, device_id={"lev": floor + 1}, device_id_type=pl.DeviceIdType.MESH
        )

    pairs = (
        (spec_hbm, spec_ref), (wave_hbm, wave_ref), (share_hbm, share_ref),
        (perm_hbm, perm_ref), (quad_hbm, quad_ref), (cor_hbm, cor_ref),
    )
    brought = [
        pltpu.make_async_copy(source, target, in_sem.at[k])
        for k, (source, target) in enumerate(pairs)
    ]
    for copy in brought:
        copy.start()
    loads = []
    for slot in range(slots):
        for hemi in range(2):
            piece = pl.ds(hemi * half, half)
            loads.append(
                pltpu.make_async_copy(
                    leg_hbm.at[slot, piece], leg.at[slot, piece], load_sem.at[slot * 2 + hemi]
                )
            )
    for hemi in range(2):
        for slot in range(slots):
            loads[slot * 2 + hemi].start()
    for copy in brought:
        copy.wait()
    degree = lax.broadcasted_iota(jnp.int32, (1, degrees), 1)
    live = [
        jnp.where(degree < degrees - wave_ref[slot], 1.0, 0.0).astype(jnp.float32)
        for slot in range(slots)
    ]
    row = lax.broadcasted_iota(jnp.int32, (8, LANES), 0)
    own = jnp.zeros((8, LANES), jnp.float32)
    for slot in range(slots):
        own = jnp.where(row == slot, wave_ref[slot].astype(jnp.float32), own)
    wave_send[...] = own
    geo[...] = jnp.zeros_like(geo)
    fulls = []
    for slot in range(slots):
        full = spec_ref[slot].astype(jnp.float32) * live[slot]
        fulls.append(full)
        for part in range(2):
            first = part * fields * layers
            total = jnp.zeros((1, degrees), jnp.float32)
            for layer in reversed(range(layers)):
                at = first + 3 * layers + layer
                total = total + full[at : at + 1] * share_ref[layer]
                at = first + 2 * layers + layer
                geo[slot, at : at + 1, :] = total
            at = slot * 2 + part
            sum_send[at : at + 1, :] = total
    place = lax.broadcasted_iota(jnp.int32, (1, LANES), 1) // (LANES // slots)
    gain = jnp.ones((1, LANES), jnp.float32)
    for slot in range(slots):
        twice = jnp.where(wave_ref[slot] == 0, 1.0, 2.0)
        gain = jnp.where(place == slot, twice, gain)
    fourier_stage(dims, fulls, leg, loads, gain, rows)
    split_rows(dims, rows, send)
    pl.semaphore_wait(barrier, groups - 1 + jnp.where(floor > 0, 1, 0))

    def wave_place(device):
        return wave_recv.at[pl.ds(pl.multiple_of(device * 8, 8), 8)]

    tell = exchange("wave", lambda _: wave_send, wave_place, tell_sem)
    lift = [
        pltpu.make_async_remote_copy(
            src_ref=sum_recv.at[step - 1] if step else sum_send,
            dst_ref=sum_recv.at[step],
            send_sem=sem_c.at[step],
            recv_sem=sem_d.at[step],
            device_id={"lev": lax.rem(floor + floors - 1, floors)},
            device_id_type=pl.DeviceIdType.MESH,
        )
        for step in range(floors - 1)
    ]

    def raise_sums(step):
        if step:

            @pl.when(floor + step < floors)
            def _():
                lift[step - 1].wait_recv()

        if step < floors - 1:

            @pl.when((floor > 0) & (floor + step < floors))
            def _():
                lift[step].start()

    for copy in tell:
        copy.start()
    wave_recv[pl.ds(pl.multiple_of(me * 8, 8), 8), :] = own
    there = exchange("wave", lambda p: send.at[p], lambda p: recv.at[p], there_sem)
    for copy in there:
        copy.start()
    raise_sums(0)
    recv[me] = send[me]
    partner, state, hop, tab, back_tab, cor, scale, base, total = scratch
    prepare_stage(dims, me, degrees, quad_ref, cor_ref, partner, cor, scale)
    tiles = tile_list(dims, me)
    others = pl.ds(0, groups - 1)
    several = pl.ds(0, (groups - 1) * 8)
    told = all_of("wave", wave_recv.at[several], wave_recv.at[several], tell_sem)
    told.wait()
    waves = [wave_recv[pl.ds(slot, groups, stride=8), :] for slot in range(slots)]
    base_stage(dims, me, waves, partner, state, hop)
    raise_sums(1)
    fill_stage(dims, me, tiles, state, hop, tab, back_tab)
    all_of("wave", send.at[others], recv.at[others], there_sem).wait()
    for source in range(groups):
        get[source * count : (source + 1) * count, :] = recv[source].astype(jnp.float32)
    coefficient_stage(dims, get, base, total)
    if floors > 2:
        raise_sums(2)
    item_stage(dims, me, tiles, state, hop, base, tab, back_tab, cor, total)
    return_stage(dims, total, scale, (north, south))
    hemi = lax.broadcasted_iota(jnp.int32, (count, LANES), 1) // layers % 2
    for source in range(groups):
        piece = slice(source * count, (source + 1) * count)
        back_send[source] = jnp.where(hemi == 1, south[piece], north[piece]).astype(jnp.bfloat16)
    home = exchange("wave", lambda p: back_send.at[p], lambda p: back.at[p], home_sem)
    for copy in home:
        copy.start()
    back[me] = back_send[me]
    for step in range(3, floors):
        raise_sums(step)
    for step in range(floors - 1):

        @pl.when((floor > 0) & (floor + step < floors))
        def _():
            lift[step].wait_send()

    for slot in range(slots):
        for part in range(2):
            at = slot * 2 + part
            deeper = jnp.zeros((1, degrees), jnp.float32)
            for step in range(floors - 1):
                value = sum_recv[step, at : at + 1, :]
                deeper = deeper + jnp.where(floor + step + 1 < floors, value, 0.0)
            first = (part * fields + 2) * layers
            geo[slot, first : first + layers, :] += deeper
    all_of("wave", back_send.at[others], back.at[others], home_sem).wait()
    pieces = [piece.astype(jnp.float32) for piece in joined_rows(dims, back)]
    joined = jnp.concatenate(pieces, 0).astype(jnp.bfloat16)
    for slot, value in enumerate(final_stage(dims, joined, leg, perm_ref)):
        out_ref[slot] = ((value + geo[slot]) * live[slot]).astype(jnp.bfloat16)


def body(spec, legendre, layer_depth_share, quad_weight, wave_of_slot):
    slots, columns, degrees = spec.shape
    total_lat = legendre.shape[1]
    groups = lax.axis_size("wave")
    layers = layer_depth_share.shape[0]
    quarter = total_lat // groups // 4
    depth = 2 * slots * groups
    block = max(b for b in range(1, quarter + 1) if quarter % b == 0 and b * depth <= max(256, depth))
    dims = dict(
        slots=slots, columns=columns, half=total_lat // 2, groups=groups, layers=layers,
        fields=columns // (2 * layers), quarter=quarter, block=block, waves=slots * groups,
    )
    fields = dims["fields"]
    maps = lane_maps(slots, fields, layers)
    perm = np.zeros((LANES, LANES), np.float32)
    perm[maps, np.arange(LANES)] = 1.0
    perm = jnp.asarray(perm, jnp.bfloat16)
    lat = np.arange(total_lat)
    coriolis = jnp.asarray(2.0 * np.cos(np.pi * (lat + 0.5) / total_lat), jnp.float32)
    floors = lax.axis_size("lev")
    half, count = total_lat // 2, 2 * quarter
    vmem = pl.BlockSpec(memory_space=pltpu.VMEM)
    rows = pltpu.VMEM((groups, count, LANES), jnp.bfloat16)
    flat = pltpu.VMEM((groups * count, LANES), jnp.float32)
    sums = 2 * slots
    operands = (spec, legendre, perm, layer_depth_share, quad_weight, coriolis, wave_of_slot)
    operands = [pltpu.with_memory_space_constraint(x, pltpu.HBM) for x in operands]
    return pl.pallas_call(
        functools.partial(whole_kernel, dims),
        out_shape=jax.ShapeDtypeStruct(spec.shape, jnp.bfloat16),
        in_specs=[pl.BlockSpec(memory_space=pltpu.HBM)] * len(operands),
        out_specs=vmem,
        scratch_shapes=[
            pltpu.VMEM(spec.shape, jnp.bfloat16),
            pltpu.VMEM((LANES, LANES), jnp.bfloat16),
            pltpu.SMEM(layer_depth_share.shape, jnp.float32),
            pltpu.SMEM(quad_weight.shape, jnp.float32),
            pltpu.SMEM(quad_weight.shape, jnp.float32),
            pltpu.SMEM(wave_of_slot.shape, jnp.int32),
            pltpu.SemaphoreType.DMA((6,)),
            pltpu.VMEM(legendre.shape, jnp.bfloat16),
            pltpu.VMEM((half, LANES), jnp.float32),
            rows, rows, rows, rows,
            pltpu.VMEM((8, LANES), jnp.float32),
            pltpu.VMEM((groups * 8, LANES), jnp.float32),
            pltpu.VMEM((sums, degrees), jnp.float32),
            pltpu.VMEM((floors, sums, degrees), jnp.float32),
            pltpu.VMEM(spec.shape, jnp.float32),
            flat, flat, flat,
            pltpu.SemaphoreType.DMA((2 * slots,)),
            pltpu.SemaphoreType.DMA((2,)),
            pltpu.SemaphoreType.DMA((floors - 1,)),
            pltpu.SemaphoreType.DMA((floors - 1,)),
            pltpu.SemaphoreType.DMA((2,)),
            pltpu.SemaphoreType.DMA((2,)),
        ]
        + grid_scratch(dims),
        compiler_params=pltpu.CompilerParams(collective_id=0, has_side_effects=True, vmem_limit_bytes=VMEM_BYTES),
    )(*operands)


def solution(mesh):
    in_specs = (P("wave", "lev", None), P("wave", None, None), P("lev"), P(), P("wave"))
    out_specs = P("wave", "lev", None)
    return jax.shard_map(body, mesh=mesh, in_specs=in_specs, out_specs=out_specs, check_vma=False)
```

```python
import functools
import math

import jax
import jax.numpy as jnp
import numpy as np
from jax import lax
from jax.experimental import pallas as pl
from jax.experimental.pallas import tpu as pltpu
from jax.sharding import PartitionSpec as P

LANES = 128
POINTS = 2 * LANES
UNROLL = 32
FILLS = 8
VMEM_BYTES = 48 * 2**20
NT = (((1,), (1,)), ((), ()))


def taylor(first, count):
    return [(-1.0) ** k / math.factorial(2 * k + first) for k in range(count)]


def horner(square, terms):
    total = jnp.full_like(square, terms[-1])
    for term in reversed(terms[:-1]):
        total = total * square + term
    return total


def turn_trig(steps, length, inverse):
    whole = jnp.floor(steps * inverse + 0.5)
    angle = (steps - whole * length) * (inverse * math.pi)
    square = angle * angle
    sine = angle * horner(square, taylor(1, 6))
    twice = sine + sine
    return 1.0 - twice * sine, twice * horner(square, taylor(0, 7))


def lane_maps(slots, fields, layers):
    order = np.arange(slots * 2 * 2 * fields * layers)
    natural = order.reshape(slots, 2, 2, fields, layers)
    return natural.transpose(0, 2, 3, 1, 4).reshape(-1)


def spread_rows(dims, hemi, masked):
    layers = dims["layers"]
    row = lax.broadcasted_iota(jnp.int32, (2 * layers, masked.shape[1]), 0)
    keep = row // layers == hemi
    pieces = []
    for at in range(0, masked.shape[0], 2 * layers):
        here = masked[at : at + 2 * layers]
        turned = pltpu.roll(here, layers, 0)
        pieces += [turned, here] if hemi else [here, turned]
    return jnp.concatenate([jnp.where(keep, piece, 0.0) for piece in pieces], 0)


def fourier_stage(dims, full, leg_ref, loads, gain, rows_ref):
    slots, half = dims["slots"], dims["half"]
    total = 0.0
    for hemi in range(2):
        weights = []
        for slot in range(slots):
            mine = spread_rows(dims, hemi, full[slot]).astype(jnp.bfloat16)
            blank = jnp.zeros_like(mine)
            weights.append(
                jnp.concatenate([mine if k == slot else blank for k in range(slots)], 1)
            )
        weights = jnp.concatenate(weights, 0)
        for slot in range(slots):
            loads[slot * 2 + hemi].wait()
        table = [leg_ref[slot, hemi * half : (hemi + 1) * half, :] for slot in range(slots)]
        total += lax.dot_general(
            jnp.concatenate(table, 1), weights, NT, preferred_element_type=jnp.float32
        )
    rows_ref[...] = total * gain


def split_rows(dims, rows_ref, send_ref):
    quarter, half = dims["quarter"], dims["half"]
    for place in range(dims["groups"]):
        low = rows_ref[place * quarter : (place + 1) * quarter, :]
        top = half - place * quarter
        high = rows_ref[top - quarter : top, :]
        send_ref[place] = jnp.concatenate([low, high], 0).astype(jnp.bfloat16)


def whereabouts(dims, device, number):
    quarter, block = dims["quarter"], dims["block"]
    local = [number * block + u for u in range(block)]
    dist = [
        jnp.where(
            r < quarter, device * quarter + r, dims["half"] - (device + 2) * quarter + r
        )
        for r in local
    ]
    lengths = [20 + 4 * q for q in dist]
    return local, dist, lengths, [length.astype(jnp.float32) for length in lengths]


def tiles_of(longest):
    return (longest // 2 + POINTS) // POINTS


def most_tiles(dims):
    quarter, block, half = dims["quarter"], dims["block"], dims["half"]
    most = 0
    for device in range(dims["groups"]):
        total = 0
        for number in range(2 * quarter // block):
            r = number * block + block - 1
            q = device * quarter + r if r < quarter else half - (device + 2) * quarter + r
            total += tiles_of(20 + 4 * q)
        most = max(most, total)
    return most


def back_home(dims, part, slot, u):
    width = 2 * dims["waves"]
    if width >= LANES:
        return u * width + part * dims["waves"] + slot * dims["groups"]
    share = LANES // width
    inner = (part * dims["slots"] + slot) * share + u % share
    return u // share * LANES + inner * dims["groups"]


def lane_middle(value):
    return jnp.broadcast_to(value[:, LANES // 2 : LANES // 2 + 1], value.shape)


def prepare_stage(dims, device, degrees, quad_ref, cor_ref, partner, cor, scale):
    groups, half, quarter = dims["groups"], dims["half"], dims["quarter"]
    layers, block = dims["layers"], dims["block"]
    total_lat, count = 2 * half, 2 * quarter
    row = lax.broadcasted_iota(jnp.int32, (count, LANES), 0)
    dist = row + jnp.where(row < quarter, device * quarter, half - (device + 2) * quarter)
    length = (20 + 4 * dist).astype(jnp.float32)
    inverse = 1.0 / length
    lane = lax.broadcasted_iota(jnp.int32, (count, LANES), 1)
    cosine, sine = turn_trig(((degrees - 1) * lane).astype(jnp.float32), length, inverse)
    mid_cos, mid_sin = lane_middle(cosine), lane_middle(sine)
    partner[0], partner[1] = cosine, sine
    partner[2] = mid_cos * mid_cos - mid_sin * mid_sin
    partner[3] = 2.0 * mid_cos * mid_sin
    partner[4] = inverse
    north_row = lax.broadcasted_iota(jnp.int32, (2 * layers, LANES), 0) < layers
    wave_row = lax.broadcasted_iota(jnp.int32, (2 * layers, POINTS), 0) < layers
    width = 2 * dims["waves"]
    column = lax.broadcasted_iota(jnp.int32, (2 * layers, POINTS), 1)
    if width >= LANES:
        owner = column // width
    else:
        share = LANES // width
        owner = column // LANES * share + column // groups % share

    def group(number, carry):
        _, dist, _, floats = whereabouts(dims, device, number)
        scaled = jnp.zeros((2 * layers, POINTS), jnp.float32)
        for u, length in enumerate(floats):
            cor[number, u * 2 * layers : (u + 1) * 2 * layers, :] = jnp.where(
                north_row, cor_ref[dist[u]], cor_ref[total_lat - 1 - dist[u]]
            )
            here = jnp.where(wave_row, quad_ref[dist[u]], quad_ref[total_lat - 1 - dist[u]])
            scaled = jnp.where(owner == u, here / length, scaled)
        scale[number] = scaled
        return carry

    lax.fori_loop(0, count // block, group, 0)


def base_stage(dims, device, waves, partner, state, hop):
    groups, block = dims["groups"], dims["block"]
    lane = lax.broadcasted_iota(jnp.int32, (groups, LANES), 1).astype(jnp.float32)
    number = 2 * dims["quarter"] // block
    pace = 5 if number % 5 == 0 else 1

    def group(step, carry):
        for n in [step * pace + k for k in range(pace)]:
            floats = whereabouts(dims, device, n)[3]
            for u, length in enumerate(floats):
                full_cos, full_sin, jump_cos, jump_sin, inverse = [
                    jnp.broadcast_to(partner[k, pl.ds(n * block + u, 1), :], (groups, LANES))
                    for k in range(5)
                ]
                cosine, sine = turn_trig(waves[0] * lane, length, inverse)
                mid_cos, mid_sin = lane_middle(cosine), lane_middle(sine)
                turn_cos = mid_cos * mid_cos - mid_sin * mid_sin
                turn_sin = 2.0 * mid_cos * mid_sin
                keep = [jnp.where(2.0 * wave < length, 1.0, 0.0) for wave in waves]
                rows = slice(u * groups, (u + 1) * groups)
                state[n, 0, rows, :] = cosine * keep[0]
                state[n, 1, rows, :] = sine * keep[0]
                hop[n, 0, rows, :] = turn_cos
                hop[n, 1, rows, :] = turn_sin
                rows = slice((block + u) * groups, (block + u + 1) * groups)
                state[n, 0, rows, :] = (full_cos * cosine + full_sin * sine) * keep[1]
                state[n, 1, rows, :] = (full_sin * cosine - full_cos * sine) * keep[1]
                hop[n, 0, rows, :] = jump_cos * turn_cos + jump_sin * turn_sin
                hop[n, 1, rows, :] = jump_sin * turn_cos - jump_cos * turn_sin
        return carry

    lax.fori_loop(0, number // pace, group, 0)


def tile_list(dims, device):
    sizes = [
        tiles_of(whereabouts(dims, device, n)[2][-1])
        for n in range(2 * dims["quarter"] // dims["block"])
    ]
    ends = []
    for size in sizes:
        ends.append(size + (ends[-1] if ends else 0))
    return sizes, ends


def tile_at(tiles, item):
    number, start = 0, 0
    for size, end in zip(*tiles):
        number = number + jnp.where(item >= end, 1, 0)
        start = start + jnp.where(item >= end, size, 0)
    return number, item - start


def fill_tile(dims, device, tiles, item, place, state, hop, tab, back_tab):
    slots, groups, block = dims["slots"], dims["groups"], dims["block"]
    pair = min(2, block)
    wide = slots * block * groups
    sides = POINTS // LANES
    number, index = tile_at(tiles, item)
    length = whereabouts(dims, device, number)[3][0]
    lane = lax.broadcasted_iota(jnp.int32, (groups, LANES), 1).astype(jnp.float32)
    weight = []
    for side in range(sides):
        point = lane + (index * POINTS + side * LANES).astype(jnp.float32)
        start = jnp.minimum(point + 0.5, 1.0)
        reach = (0.5 * length + 0.5) - point
        each = [jnp.maximum(jnp.minimum(reach + 2.0 * u, start), 0.0) for u in range(block)]
        weight.append(
            [
                jnp.concatenate(each[u : u + pair], 0)
                for u in range(0, block, pair)
            ]
        )
    for u in range(0, block, pair):
        for slot in range(slots):
            at = (slot * block + u) * groups
            rows = slice(at, at + pair * groups)
            cosine, sine = state[number, 0, rows, :], state[number, 1, rows, :]
            turn_cos, turn_sin = hop[number, 0, rows, :], hop[number, 1, rows, :]
            for side in range(sides):
                for part, value in enumerate((cosine, sine)):
                    put = part * wide + at
                    tab[place, side, put : put + pair * groups, :] = value.astype(jnp.bfloat16)
                    put = back_home(dims, part, slot, u)
                    back_tab[place, side, put : put + pair * groups, :] = (
                        value * weight[side][u // pair]
                    ).astype(jnp.bfloat16)
                cosine, sine = (
                    cosine * turn_cos - sine * turn_sin,
                    sine * turn_cos + cosine * turn_sin,
                )
            state[number, 0, rows, :] = cosine
            state[number, 1, rows, :] = sine


def fill_stage(dims, device, tiles, state, hop, tab, back_tab):
    def body(step, carry):
        for k in range(FILLS):
            item = step * FILLS + k
            fill_tile(dims, device, tiles, item, item, state, hop, tab, back_tab)
        return carry

    lax.fori_loop(0, (tiles[1][-1] + FILLS - 1) // FILLS, body, 0)


def coefficient_stage(dims, get_ref, base):
    slots, groups, layers = dims["slots"], dims["groups"], dims["layers"]
    fields, block, count = dims["fields"], dims["block"], 2 * dims["quarter"]
    width = fields * 2 * layers
    number = count // block
    lane = lax.broadcasted_iota(jnp.int32, (groups, LANES), 1)
    south_lane = lane // layers % 2 == 1
    first_slot = lax.broadcasted_iota(jnp.int32, (width, LANES), 1) < block * groups
    eye = (
        lax.broadcasted_iota(jnp.int32, (LANES, LANES), 0)
        == lax.broadcasted_iota(jnp.int32, (LANES, LANES), 1)
    ).astype(jnp.bfloat16)
    for start in range(0, number, 2):
        pieces = []
        for n in range(start, min(start + 2, number)):
            both = []
            for u in range(block):
                at = n * block + u
                north = get_ref[pl.ds(at, groups, stride=count), :]
                south = get_ref[pl.ds(count - 1 - at, groups, stride=count), :]
                both.append(jnp.where(south_lane, south, north))
            pieces += both * (LANES // (block * groups))
        turned = lax.dot_general(
            eye,
            jnp.concatenate(pieces, 0).astype(jnp.bfloat16),
            NT,
            preferred_element_type=jnp.float32,
        )
        for n in range(start, min(start + 2, number)):
            here = turned[:, (n - start) * LANES : (n - start + 1) * LANES]
            for part in range(2):
                value = [
                    here[(slot * 2 + part) * width : (slot * 2 + part + 1) * width]
                    for slot in range(slots)
                ]
                value = jnp.where(first_slot, value[0], value[1])
                base[n, part] = value.astype(jnp.bfloat16)


def side_by_side(ref, index):
    return jnp.concatenate([ref[index, side] for side in range(ref.shape[1])], 1)


def item_stage(dims, device, tiles, state, hop, base, tab, back_tab, cor, total):
    groups, layers, block = dims["groups"], dims["layers"], dims["block"]
    fields = dims["fields"]
    width = fields * 2 * layers
    rows = 2 * width
    lane = lax.broadcasted_iota(jnp.int32, (width, LANES), 1)
    mine = [
        (lane // groups % block == u).astype(jnp.float32).astype(jnp.bfloat16)
        for u in range(block)
    ]
    span = 2 * dims["waves"]
    share = max(1, LANES // span)
    reach = max(LANES, span)
    across = lax.broadcasted_iota(jnp.int32, (width, reach), 1)
    sign = jnp.where(across // (reach // 2) == 0, 1.0, -1.0)

    def one(item, place):
        n = tile_at(tiles, item)[0]
        pieces = []
        for u in range(block):
            left, right = base[n, 0] * mine[u], base[n, 1] * mine[u]
            pieces.append(jnp.concatenate([left, -right], 1))
            pieces.append(jnp.concatenate([left, right], 1))
        grid = jnp.dot(
            jnp.concatenate(pieces, 0),
            side_by_side(tab, place),
            preferred_element_type=jnp.float32,
        )
        made = []
        for u in range(block):
            extra = cor[n, u * 2 * layers : (u + 1) * 2 * layers, :]
            extra = jnp.concatenate([extra] * (POINTS // LANES), 1)
            for side in range(2):
                at = (u * 2 + side) * width
                part = [
                    grid[at + f * 2 * layers : at + (f + 1) * 2 * layers] for f in range(fields)
                ]
                absolute = part[2] + extra
                made += [
                    absolute * part[0],
                    absolute * part[1],
                    0.5 * (part[0] * part[0] + part[1] * part[1]),
                    part[0] * part[3],
                ]
        products = jnp.concatenate(made, 0).astype(jnp.bfloat16)
        back = lax.dot_general(
            products, side_by_side(back_tab, place), NT, preferred_element_type=jnp.float32
        )
        for start in range(0, block, share):
            column = start * span // LANES * LANES
            joined = jnp.zeros((width, reach), jnp.float32)
            for u in range(start, min(start + share, block)):
                near = back[u * rows : u * rows + width, column : column + reach]
                far = back[u * rows + width : (u + 1) * rows, column : column + reach]
                value = near * sign + far
                keep = across // groups % share == u - start
                joined = value if share == 1 else jnp.where(keep, value, joined)
            total[n, :, column : column + reach] += joined

    def body(step, carry):
        for k in range(UNROLL):
            item = step * UNROLL + k
            one(item, item)
        return carry

    lax.fori_loop(0, (tiles[1][-1] + UNROLL - 1) // UNROLL, body, 0)


def return_stage(dims, total, scale, put_refs):
    slots, groups, layers = dims["slots"], dims["groups"], dims["layers"]
    fields, block, count = dims["fields"], dims["block"], 2 * dims["quarter"]
    width, span = fields * 2 * layers, 2 * dims["waves"]
    number = count // block
    share = max(1, LANES // span)
    lane = lax.broadcasted_iota(jnp.int32, (block * groups, POINTS), 1)
    row = lax.broadcasted_iota(jnp.int32, (block * groups, POINTS), 0)
    if span >= LANES:
        owner, kind = lane // span, lane % span // groups
    else:
        owner = lane // LANES * share + lane // groups % share
        kind = lane % LANES // (groups * share)
    pick = (owner * groups + lane % groups == row).astype(jnp.float32).astype(jnp.bfloat16)
    keep = []
    for slot in range(slots):
        for part in range(2):
            at = (kind[:1] == part * slots + slot).astype(jnp.float32)
            keep.append(jnp.broadcast_to(at, (width, POINTS)).astype(jnp.bfloat16))
    for start in range(0, number, 2):
        pieces = []
        for n in range(start, min(start + 2, number)):
            value = total[n] * jnp.concatenate([scale[n]] * fields, 0)
            value = value.astype(jnp.bfloat16)
            pieces += [value * here for here in keep]
        turned = lax.dot_general(
            pick, jnp.concatenate(pieces, 0), NT, preferred_element_type=jnp.float32
        )
        for n in range(start, min(start + 2, number)):
            for u in range(block):
                at = n * block + u
                value = turned[
                    u * groups : (u + 1) * groups, (n - start) * LANES : (n - start + 1) * LANES
                ]
                put_refs[0][pl.ds(at, groups, stride=count), :] = value
                put_refs[1][pl.ds(count - 1 - at, groups, stride=count), :] = value


def grid_scratch(dims):
    slots, groups, block = dims["slots"], dims["groups"], dims["block"]
    layers, fields = dims["layers"], dims["fields"]
    number = 2 * dims["quarter"] // block
    wide = slots * block * groups
    width = fields * 2 * layers
    items = -(-most_tiles(dims) // UNROLL) * UNROLL
    return [
        pltpu.VMEM((5, number * block, LANES), jnp.float32),
        pltpu.VMEM((number + 1, 2, wide, LANES), jnp.float32),
        pltpu.VMEM((number + 1, 2, wide, LANES), jnp.float32),
        pltpu.VMEM((items, POINTS // LANES, 2 * wide, LANES), jnp.bfloat16),
        pltpu.VMEM((items, POINTS // LANES, 2 * wide, LANES), jnp.bfloat16),
        pltpu.VMEM((number + 1, block * 2 * layers, LANES), jnp.float32),
        pltpu.VMEM((number, 2 * layers, POINTS), jnp.float32),
        pltpu.VMEM((number + 1, 2, width, wide), jnp.bfloat16),
        pltpu.VMEM((number + 1, width, 2 * wide), jnp.float32),
    ]


def final_stage(dims, get, leg_ref, perm_ref):
    slots, columns = dims["slots"], dims["columns"]
    turned = lax.dot_general(
        perm_ref[...], get, NT, preferred_element_type=jnp.float32
    ).astype(jnp.bfloat16)
    results = []
    for slot in range(slots):
        rows = [
            turned[(slot * 2 + hemi) * columns : (slot * 2 + hemi + 1) * columns]
            for hemi in range(2)
        ]
        total = jnp.dot(
            jnp.concatenate(rows, 1), leg_ref[slot], preferred_element_type=jnp.float32
        )
        results.append(total)
    return results


def joined_rows(dims, back_ref):
    quarter, groups = dims["quarter"], dims["groups"]
    low = [back_ref[place][:quarter] for place in range(groups)]
    high = [back_ref[place][quarter:] for place in reversed(range(groups))]
    return low + high


def to_peer(axis, shift):
    place = lax.axis_index(axis)
    count = lax.axis_size(axis)
    return {axis: lax.rem(place + shift, count)}


def far_first(count):
    if count & (count - 1):
        return list(range(1, count))
    return sorted(range(1, count), key=lambda d: (-bin(d >> 1).count("1"), d))


def partner_of(place, count, step):
    if count & (count - 1):
        return lax.rem(place + step, count)
    peer, bit = place, 1
    while bit < count:
        if step & bit:
            peer = peer + bit * (1 - 2 * lax.rem(lax.div(place, bit), 2))
        bit *= 2
    return peer


def exchange(axis, source_of, target_of, sems):
    place = lax.axis_index(axis)
    count = lax.axis_size(axis)
    copies = []
    for step in far_first(count):
        peer = partner_of(place, count, step)
        copies.append(
            pltpu.make_async_remote_copy(
                src_ref=source_of(peer),
                dst_ref=target_of(place),
                send_sem=sems.at[0],
                recv_sem=sems.at[1],
                device_id={axis: peer},
                device_id_type=pl.DeviceIdType.MESH,
            )
        )
    return copies


def all_of(axis, source, target, sems):
    return pltpu.make_async_remote_copy(
        src_ref=source,
        dst_ref=target,
        send_sem=sems.at[0],
        recv_sem=sems.at[1],
        device_id=to_peer(axis, 1),
        device_id_type=pl.DeviceIdType.MESH,
    )


def whole_kernel(
    dims, spec_hbm, leg_hbm, perm_hbm, share_hbm, quad_hbm, cor_hbm, wave_hbm, out_ref,
    spec_ref, perm_ref, share_ref, quad_ref, cor_ref, wave_ref, in_sem,
    leg, rows, send, recv, back_send, back, wave_send, wave_recv, sum_send, sum_recv, geo,
    get, north, south, load_sem, tell_sem, sem_c, sem_d, there_sem, home_sem, *scratch,
):
    slots, groups, half = dims["slots"], dims["groups"], dims["half"]
    fields, layers, count = dims["fields"], dims["layers"], 2 * dims["quarter"]
    degrees = spec_hbm.shape[2]
    me = lax.axis_index("wave")
    floor = lax.axis_index("lev")
    floors = lax.axis_size("lev")
    barrier = pltpu.get_barrier_semaphore()
    for step in far_first(groups):
        pl.semaphore_signal(
            barrier,
            inc=1,
            device_id={"wave": partner_of(me, groups, step)},
            device_id_type=pl.DeviceIdType.MESH,
        )

    @pl.when(floor < floors - 1)
    def _():
        pl.semaphore_signal(
            barrier, inc=1, device_id={"lev": floor + 1}, device_id_type=pl.DeviceIdType.MESH
        )

    pairs = (
        (spec_hbm, spec_ref), (wave_hbm, wave_ref), (share_hbm, share_ref),
        (perm_hbm, perm_ref), (quad_hbm, quad_ref), (cor_hbm, cor_ref),
    )
    brought = [
        pltpu.make_async_copy(source, target, in_sem.at[k])
        for k, (source, target) in enumerate(pairs)
    ]
    for copy in brought:
        copy.start()
    loads = []
    for slot in range(slots):
        for hemi in range(2):
            piece = pl.ds(hemi * half, half)
            loads.append(
                pltpu.make_async_copy(
                    leg_hbm.at[slot, piece], leg.at[slot, piece], load_sem.at[slot * 2 + hemi]
                )
            )
    for hemi in range(2):
        for slot in range(slots):
            loads[slot * 2 + hemi].start()
    for copy in brought:
        copy.wait()
    degree = lax.broadcasted_iota(jnp.int32, (1, degrees), 1)
    live = [
        jnp.where(degree < degrees - wave_ref[slot], 1.0, 0.0).astype(jnp.float32)
        for slot in range(slots)
    ]
    row = lax.broadcasted_iota(jnp.int32, (8, LANES), 0)
    own = jnp.zeros((8, LANES), jnp.float32)
    for slot in range(slots):
        own = jnp.where(row == slot, wave_ref[slot].astype(jnp.float32), own)
    wave_send[...] = own
    geo[...] = jnp.zeros_like(geo)
    fulls = []
    for slot in range(slots):
        full = spec_ref[slot].astype(jnp.float32) * live[slot]
        fulls.append(full)
        for part in range(2):
            first = part * fields * layers
            total = jnp.zeros((1, degrees), jnp.float32)
            for layer in reversed(range(layers)):
                at = first + 3 * layers + layer
                total = total + full[at : at + 1] * share_ref[layer]
                at = first + 2 * layers + layer
                geo[slot, at : at + 1, :] = total
            at = slot * 2 + part
            sum_send[at : at + 1, :] = total
    place = lax.broadcasted_iota(jnp.int32, (1, LANES), 1) // (LANES // slots)
    gain = jnp.ones((1, LANES), jnp.float32)
    for slot in range(slots):
        twice = jnp.where(wave_ref[slot] == 0, 1.0, 2.0)
        gain = jnp.where(place == slot, twice, gain)
    fourier_stage(dims, fulls, leg, loads, gain, rows)
    split_rows(dims, rows, send)
    pl.semaphore_wait(barrier, groups - 1 + jnp.where(floor > 0, 1, 0))

    def wave_place(device):
        return wave_recv.at[pl.ds(pl.multiple_of(device * 8, 8), 8)]

    tell = exchange("wave", lambda _: wave_send, wave_place, tell_sem)
    lift = [
        pltpu.make_async_remote_copy(
            src_ref=sum_recv.at[step - 1] if step else sum_send,
            dst_ref=sum_recv.at[step],
            send_sem=sem_c.at[step],
            recv_sem=sem_d.at[step],
            device_id={"lev": lax.rem(floor + floors - 1, floors)},
            device_id_type=pl.DeviceIdType.MESH,
        )
        for step in range(floors - 1)
    ]

    def raise_sums(step):
        if step:

            @pl.when(floor + step < floors)
            def _():
                lift[step - 1].wait_recv()

        if step < floors - 1:

            @pl.when((floor > 0) & (floor + step < floors))
            def _():
                lift[step].start()

    for copy in tell:
        copy.start()
    wave_recv[pl.ds(pl.multiple_of(me * 8, 8), 8), :] = own
    there = exchange("wave", lambda p: send.at[p], lambda p: recv.at[p], there_sem)
    for copy in there:
        copy.start()
    raise_sums(0)
    recv[me] = send[me]
    partner, state, hop, tab, back_tab, cor, scale, base, total = scratch
    prepare_stage(dims, me, degrees, quad_ref, cor_ref, partner, cor, scale)
    total[...] = jnp.zeros_like(total)
    tiles = tile_list(dims, me)
    others = pl.ds(0, groups - 1)
    several = pl.ds(0, (groups - 1) * 8)
    told = all_of("wave", wave_recv.at[several], wave_recv.at[several], tell_sem)
    told.wait()
    waves = [wave_recv[pl.ds(slot, groups, stride=8), :] for slot in range(slots)]
    base_stage(dims, me, waves, partner, state, hop)
    raise_sums(1)
    fill_stage(dims, me, tiles, state, hop, tab, back_tab)
    all_of("wave", send.at[others], recv.at[others], there_sem).wait()
    for source in range(groups):
        get[source * count : (source + 1) * count, :] = recv[source].astype(jnp.float32)
    coefficient_stage(dims, get, base)
    if floors > 2:
        raise_sums(2)
    item_stage(dims, me, tiles, state, hop, base, tab, back_tab, cor, total)
    return_stage(dims, total, scale, (north, south))
    hemi = lax.broadcasted_iota(jnp.int32, (count, LANES), 1) // layers % 2
    for source in range(groups):
        piece = slice(source * count, (source + 1) * count)
        back_send[source] = jnp.where(hemi == 1, south[piece], north[piece]).astype(jnp.bfloat16)
    home = exchange("wave", lambda p: back_send.at[p], lambda p: back.at[p], home_sem)
    for copy in home:
        copy.start()
    back[me] = back_send[me]
    for step in range(3, floors):
        raise_sums(step)
    for step in range(floors - 1):

        @pl.when((floor > 0) & (floor + step < floors))
        def _():
            lift[step].wait_send()

    for slot in range(slots):
        for part in range(2):
            at = slot * 2 + part
            deeper = jnp.zeros((1, degrees), jnp.float32)
            for step in range(floors - 1):
                value = sum_recv[step, at : at + 1, :]
                deeper = deeper + jnp.where(floor + step + 1 < floors, value, 0.0)
            first = (part * fields + 2) * layers
            geo[slot, first : first + layers, :] += deeper
    all_of("wave", back_send.at[others], back.at[others], home_sem).wait()
    pieces = [piece.astype(jnp.float32) for piece in joined_rows(dims, back)]
    joined = jnp.concatenate(pieces, 0).astype(jnp.bfloat16)
    for slot, value in enumerate(final_stage(dims, joined, leg, perm_ref)):
        out_ref[slot] = ((value + geo[slot]) * live[slot]).astype(jnp.bfloat16)


def body(spec, legendre, layer_depth_share, quad_weight, wave_of_slot):
    slots, columns, degrees = spec.shape
    total_lat = legendre.shape[1]
    groups = lax.axis_size("wave")
    layers = layer_depth_share.shape[0]
    quarter = total_lat // groups // 4
    depth = 2 * slots * groups
    block = max(b for b in range(1, quarter + 1) if quarter % b == 0 and b * depth <= max(256, depth))
    dims = dict(
        slots=slots, columns=columns, half=total_lat // 2, groups=groups, layers=layers,
        fields=columns // (2 * layers), quarter=quarter, block=block, waves=slots * groups,
    )
    fields = dims["fields"]
    maps = lane_maps(slots, fields, layers)
    perm = np.zeros((LANES, LANES), np.float32)
    perm[maps, np.arange(LANES)] = 1.0
    perm = jnp.asarray(perm, jnp.bfloat16)
    lat = np.arange(total_lat)
    coriolis = jnp.asarray(2.0 * np.cos(np.pi * (lat + 0.5) / total_lat), jnp.float32)
    floors = lax.axis_size("lev")
    half, count = total_lat // 2, 2 * quarter
    vmem = pl.BlockSpec(memory_space=pltpu.VMEM)
    rows = pltpu.VMEM((groups, count, LANES), jnp.bfloat16)
    flat = pltpu.VMEM((groups * count, LANES), jnp.float32)
    sums = 2 * slots
    operands = (spec, legendre, perm, layer_depth_share, quad_weight, coriolis, wave_of_slot)
    operands = [pltpu.with_memory_space_constraint(x, pltpu.HBM) for x in operands]
    return pl.pallas_call(
        functools.partial(whole_kernel, dims),
        out_shape=jax.ShapeDtypeStruct(spec.shape, jnp.bfloat16),
        in_specs=[pl.BlockSpec(memory_space=pltpu.HBM)] * len(operands),
        out_specs=vmem,
        scratch_shapes=[
            pltpu.VMEM(spec.shape, jnp.bfloat16),
            pltpu.VMEM((LANES, LANES), jnp.bfloat16),
            pltpu.SMEM(layer_depth_share.shape, jnp.float32),
            pltpu.SMEM(quad_weight.shape, jnp.float32),
            pltpu.SMEM(quad_weight.shape, jnp.float32),
            pltpu.SMEM(wave_of_slot.shape, jnp.int32),
            pltpu.SemaphoreType.DMA((6,)),
            pltpu.VMEM(legendre.shape, jnp.bfloat16),
            pltpu.VMEM((half, LANES), jnp.float32),
            rows, rows, rows, rows,
            pltpu.VMEM((8, LANES), jnp.float32),
            pltpu.VMEM((groups * 8, LANES), jnp.float32),
            pltpu.VMEM((sums, degrees), jnp.float32),
            pltpu.VMEM((floors, sums, degrees), jnp.float32),
            pltpu.VMEM(spec.shape, jnp.float32),
            flat, flat, flat,
            pltpu.SemaphoreType.DMA((2 * slots,)),
            pltpu.SemaphoreType.DMA((2,)),
            pltpu.SemaphoreType.DMA((floors - 1,)),
            pltpu.SemaphoreType.DMA((floors - 1,)),
            pltpu.SemaphoreType.DMA((2,)),
            pltpu.SemaphoreType.DMA((2,)),
        ]
        + grid_scratch(dims),
        compiler_params=pltpu.CompilerParams(collective_id=0, has_side_effects=True, vmem_limit_bytes=VMEM_BYTES),
    )(*operands)


def solution(mesh):
    in_specs = (P("wave", "lev", None), P("wave", None, None), P("lev"), P(), P("wave"))
    out_specs = P("wave", "lev", None)
    return jax.shard_map(body, mesh=mesh, in_specs=in_specs, out_specs=out_specs, check_vma=False)
```
